128 devices in a mesh: grp: 4 (over x_hi, core), dev: 32 (over z, y, x_lo).
Axes of the slice: x: 4 (x_hi: 2, x_lo: 2; x = x_hi * 2 + x_lo), y: 4, z: 4, core: 2. Of those that a mesh axis runs over, the one named last changes fastest.
Arguments:
- fields: float32 [24, 256, 128, 128], P(None, ('grp', 'dev')), may hold values from -6 to 6
- mix_matrix: float32 [24, 24], replicated, may hold values from -1.25 to 1.25
- laplace_matrix: float32 [24, 24], replicated, may hold values from -0.21875 to 0.21875
Outputs:
- rhs: float32 [24, 256, 128, 128], P(None, ('grp', 'dev'))
- weyl: float32 [2, 256, 128, 128], P(None, 'grp', 'dev')
The draws below stay inside these ranges and needn't reach their ends.
All inputs are finite; a program needn't handle non-finite values.
Results may differ from the reference program's by a relative error of at most 0.0003.
Values sent between devices are 32-bit elements; how exact they have to be, the bound alone decides.
A program may use at most 192 MiB of HBM per device.

```python
import jax
import jax.numpy as jnp
from jax import lax

FIELDS = 24
CZ = 2
NY = 128
NX = 128
NZ = 256


def block_scale(key, dims, split, smallest, top_value):
    level = 1.0
    for position, blocks in split:
        draws = jax.random.uniform(jax.random.fold_in(jax.random.fold_in(key, 6), position), (blocks,), jnp.float32, smallest / len(split), top_value / len(split))
        level = level * jnp.repeat(jnp.exp(draws), dims[position] // blocks).reshape((-1,) + (1,) * (len(dims) - 1 - position))
    return level


def normal_values(stream_key, shape, scale, reach, split=(), kind=jnp.bfloat16):
    values = scale * jax.random.normal(stream_key, shape, jnp.float32)
    if split:
        values = values * block_scale(stream_key, shape, split, -0.22, 0.18)
    return jnp.clip(values, -reach, reach).astype(kind)


def setup_inputs(seed: int = 0) -> dict:
    keys = jax.random.split(jax.random.key(seed), 4)
    fields = normal_values(keys[0], (FIELDS, NZ, NY, NX), 1.0, 6.0, ((1, 128),), jnp.float32)
    mix_matrix = normal_values(keys[1], (FIELDS, FIELDS), FIELDS ** -0.5, 1.25, (), jnp.float32)
    laplace_matrix = normal_values(keys[2], (FIELDS, FIELDS), (FIELDS * 30) ** -0.5, 0.21875, (), jnp.float32)
    return {"fields": fields, "mix_matrix": mix_matrix, "laplace_matrix": laplace_matrix}


def pad_periodic(field, dimension):
    length = field.shape[dimension]
    before = lax.slice_in_dim(field, length - 2, length, axis=dimension)
    after = lax.slice_in_dim(field, 0, 2, axis=dimension)
    return jnp.concatenate([before, field, after], axis=dimension)

def interior(padded, keep):
    result = padded
    for dimension in (1, 2, 3):
        if dimension != keep:
            result = lax.slice_in_dim(result, 2, result.shape[dimension] - 2, axis=dimension)
    return result

def stencil_values(padded, dimension):
    centre = interior(padded, dimension)
    length = centre.shape[dimension] - 4
    return [lax.slice_in_dim(centre, offset, offset + length, axis=dimension) for offset in range(5)]

def first_diff(padded, dimension):
    values = stencil_values(padded, dimension)
    return (values[0] - 8.0 * values[1] + 8.0 * values[3] - values[4]) / 12.0

def second_diff(padded, dimension):
    values = stencil_values(padded, dimension)
    return (-values[0] + 16.0 * values[1] - 30.0 * values[2] + 16.0 * values[3] - values[4]) / 12.0

def laplacian(padded):
    return second_diff(padded, 1) + second_diff(padded, 2) + second_diff(padded, 3)

def evolution(padded, mix_matrix, laplace_matrix):
    centre = interior(padded, 0)
    laplace = laplacian(padded)
    result = jnp.einsum('fg,gzyx->fzyx', mix_matrix, centre, precision=lax.Precision.HIGHEST)
    result = result + jnp.einsum('fg,gzyx->fzyx', laplace_matrix, laplace, precision=lax.Precision.HIGHEST)
    for dimension in (1, 2, 3):
        result = result + centre[11 + dimension][None] * first_diff(padded, dimension)
    return result

def contract(tensor, left, right):
    total = 0.0
    for first in range(3):
        for second in range(3):
            total = total + tensor[first][second] * left[first] * right[second]
    return total

def weyl_scalar(padded, zpos, ypos, xpos):
    table = ((0, 1, 2), (1, 3, 4), (2, 4, 5))
    metric = padded[0:6]
    curv_padded = padded[6:12]
    lap_metric = laplacian(metric)
    curvature = interior(curv_padded, 0)
    gradient = [first_diff(curv_padded, 3 - index) for index in range(3)]
    trace = curvature[0] + curvature[3] + curvature[5]
    electric = []
    curl = []
    for first in range(3):
        erow = []
        crow = []
        for second in range(3):
            value = -0.5 * lap_metric[table[first][second]] - trace * curvature[table[first][second]]
            for middle in range(3):
                value = value + curvature[table[first][middle]] * curvature[table[middle][second]]
            erow.append(value)
            next_one = (first + 1) % 3
            next_two = (first + 2) % 3
            crow.append(gradient[next_one][table[next_two][second]] - gradient[next_two][table[next_one][second]])
        electric.append(erow)
        curl.append(crow)
    magnetic = [[0.5 * (curl[first][second] + curl[second][first]) for second in range(3)] for first in range(3)]
    along_x = xpos[None, None, :]
    along_y = ypos[None, :, None]
    along_z = zpos[:, None, None]
    cylinder = jnp.sqrt(along_x * along_x + along_y * along_y)
    radius = jnp.sqrt(cylinder * cylinder + along_z * along_z)
    theta_vec = (along_z * along_x / (radius * cylinder), along_z * along_y / (radius * cylinder), -cylinder / radius)
    phi_vec = (-along_y / cylinder, along_x / cylinder, 0.0)
    real_part = 0.5 * (contract(electric, theta_vec, theta_vec) - contract(electric, phi_vec, phi_vec)) - contract(magnetic, theta_vec, phi_vec)
    imag_part = -contract(electric, theta_vec, phi_vec) - 0.5 * (contract(magnetic, theta_vec, theta_vec) - contract(magnetic, phi_vec, phi_vec))
    shape = curvature.shape[1:]
    return jnp.stack([jnp.broadcast_to(real_part, shape), jnp.broadcast_to(imag_part, shape)])

def centred(index, count):
    return index.astype(jnp.float32) + 0.5 - 0.5 * count

def reference(fields, mix_matrix, laplace_matrix):
    rows = fields.shape[2]
    width = fields.shape[3]
    padded = pad_periodic(pad_periodic(pad_periodic(fields, 1), 2), 3)
    ypos = centred(jnp.arange(rows, dtype=jnp.int32), rows)
    xpos = centred(jnp.arange(width, dtype=jnp.int32), width)

    def block(index):
        start = (index * CZ).astype(jnp.int32)
        window = lax.dynamic_slice_in_dim(padded, start, CZ + 4, axis=1)
        zpos = centred(start + jnp.arange(CZ, dtype=jnp.int32), NZ)
        return (evolution(window, mix_matrix, laplace_matrix), weyl_scalar(window[0:12], zpos, ypos, xpos))
    rhs_blocks, weyl_blocks = lax.map(block, jnp.arange(NZ // CZ, dtype=jnp.int32))
    rhs = jnp.transpose(rhs_blocks, (1, 0, 2, 3, 4)).reshape(FIELDS, NZ, rows, width)
    weyl = jnp.transpose(weyl_blocks, (1, 0, 2, 3, 4)).reshape(2, NZ, rows, width)
    return (rhs, weyl)
```

```python
import functools

import jax
import jax.numpy as jnp
from jax import lax
from jax.experimental import pallas as pl
from jax.experimental.pallas import tpu as pltpu
from jax.sharding import PartitionSpec as P

MESH = pl.DeviceIdType.MESH
F = 24
HALF = 12
ROWS = 8
LAG = 3
BLOCK = 12
COMPUTE = True
WEYL = True


def d12(m2, m1, p1, p2):
    return 8.0 * (p1 - m1) - (p2 - m2)


def kernel(groups, members, fields, mix, lapw, rhs, weyl, own, halo, tsum, w1, w2, wl,
           load_sem, send_p, recv_p, send_r, recv_r, send_d, wsend, wrecv, wlocal):
    depth = fields.shape[1]
    rows = fields.shape[2]
    width = fields.shape[3]
    tiles = rows // ROWS
    steps = 2 * tiles
    share = rows // members
    g = lax.axis_index("grp")
    d = lax.axis_index("dev")
    slabs = groups * members
    s = g * members + d
    odd = lax.rem(d, 2)
    partner = d + 1 - 2 * odd
    target = lax.rem(s + 2 - 4 * odd + slabs, slabs)
    target_id = {"grp": target // members, "dev": lax.rem(target, members)}
    nearby = lax.rem(s - 1 + 2 * odd + slabs, slabs)
    nearby_id = {"grp": nearby // members, "dev": lax.rem(nearby, members)}
    godd = lax.rem(g, 2)
    last = d >= members - 2
    first = d < 2
    cross = (last & (godd == 1)) | (first & (godd == 0))
    relays = jnp.logical_not(cross & ((d == members - 2) | (d == 1)))
    direct = cross & ((d == members - 1) | (d == 0))

    loads = []
    for half in range(2):
        part = pl.ds(half * HALF, HALF)
        loads.append(pltpu.make_async_copy(
            fields.at[part], own.at[part, :, pl.ds(8, rows), :], load_sem.at[half]))
    loads.append(pltpu.make_async_copy(
        fields.at[:, :, pl.ds(rows - 8, 8), :], own.at[:, :, pl.ds(0, 8), :], load_sem.at[2]))
    loads.append(pltpu.make_async_copy(
        fields.at[:, :, pl.ds(0, 8), :], own.at[:, :, pl.ds(rows + 8, 8), :], load_sem.at[3]))
    for load in loads:
        load.start()

    barrier = pltpu.get_barrier_semaphore()

    def greet(offset, _):
        pl.semaphore_signal(barrier, inc=1, device_id={"dev": lax.rem(d + offset, members)},
                            device_id_type=MESH)
        return 0

    lax.fori_loop(1, members, greet, 0)
    edge = jnp.where(last, 1, jnp.where(first, 1, 0))

    @pl.when(edge == 1)
    def _():
        other = lax.rem(g + jnp.where(last, 1, groups - 1), groups)
        base = jnp.where(last, 0, members - 2)
        for k in range(2):
            pl.semaphore_signal(barrier, inc=1, device_id={"grp": other, "dev": base + k},
                                device_id_type=MESH)

    pl.semaphore_wait(barrier, members - 1 + 2 * edge)

    def window(k):
        half = k // tiles
        tile = lax.rem(k, tiles)
        return half * HALF, tile * ROWS

    def own_chunk(k):
        f0, r0 = window(k)
        return own.at[pl.ds(f0, HALF), :, pl.ds(pl.multiple_of(r0 + 8, 8), ROWS), :]

    def halo_chunk(slot, k):
        f0, r0 = window(k)
        return halo.at[slot, pl.ds(f0, HALF), :, pl.ds(pl.multiple_of(r0, 8), ROWS), :]

    mine = 1 - odd

    def to_partner(k):
        return pltpu.make_async_remote_copy(
            own_chunk(k), halo_chunk(odd, k), send_p.at[k], recv_p.at[k],
            device_id={"dev": partner}, device_id_type=MESH)

    def from_partner(k):
        return pltpu.make_async_remote_copy(
            own_chunk(k), halo_chunk(mine, k), send_p.at[k], recv_p.at[k],
            device_id={"dev": partner}, device_id_type=MESH)

    def relay(k):
        return pltpu.make_async_remote_copy(
            halo_chunk(mine, k), halo_chunk(odd, k), send_r.at[k], recv_r.at[k],
            device_id=target_id, device_id_type=MESH)

    def straight(k):
        return pltpu.make_async_remote_copy(
            own_chunk(k), halo_chunk(mine, k), send_d.at[k], recv_r.at[k],
            device_id=nearby_id, device_id_type=MESH)

    def first_sends(k, _):
        to_partner(k).start()

        @pl.when(direct)
        def _():
            straight(k).start()
        return 0

    loads[0].wait()
    lax.fori_loop(0, tiles, first_sends, 0)
    loads[1].wait()
    lax.fori_loop(tiles, steps, first_sends, 0)
    loads[2].wait()
    loads[3].wait()

    if COMPUTE:
        def spread(at, _):
            c = at // F
            h = lax.rem(at, F)
            lap = lapw[c, h]
            w1[h, c] = jnp.full((8, 128), mix[c, h] - 7.5 * lap, jnp.float32)
            w2[h, c] = jnp.full((8, 128), lap * (1.0 / 12.0), jnp.float32)
            return 0

        lax.fori_loop(0, F * F, spread, 0)

    lane = lax.broadcasted_iota(jnp.int32, (ROWS, width), 1).astype(jnp.float32)
    line = lax.broadcasted_iota(jnp.int32, (ROWS, width), 0).astype(jnp.float32)

    def near(h, r0, p):
        def at(off):
            return own[h, p, pl.ds(r0 + 8 + off, ROWS), :]
        here = own[h, p, pl.ds(pl.multiple_of(r0 + 8, 8), ROWS), :]
        rows_at = pl.ds(pl.multiple_of(r0, 8), ROWS)
        xs = [pltpu.roll(here, 2, 1), pltpu.roll(here, 1, 1),
              pltpu.roll(here, width - 1, 1), pltpu.roll(here, width - 2, 1)]
        ys = [at(-2), at(-1), at(1), at(2)]
        if p == 0:
            zs = [halo[0, h, 0, rows_at, :], halo[0, h, 1, rows_at, :],
                  own[h, 1, pl.ds(pl.multiple_of(r0 + 8, 8), ROWS), :], halo[1, h, 0, rows_at, :]]
        else:
            zs = [halo[0, h, 1, rows_at, :],
                  own[h, 0, pl.ds(pl.multiple_of(r0 + 8, 8), ROWS), :],
                  halo[1, h, 0, rows_at, :], halo[1, h, 1, rows_at, :]]
        return here, xs, ys, zs

    def lap_sum(xs, ys, zs):
        one = (xs[1] + xs[2]) + (ys[1] + ys[2]) + (zs[1] + zs[2])
        two = (xs[0] + xs[3]) + (ys[0] + ys[3]) + (zs[0] + zs[3])
        return 16.0 * one - two

    def weyl_tile(tile):
        r0 = tile * ROWS
        xpos = lane + (0.5 - 0.5 * width)
        ypos = line + (r0.astype(jnp.float32) + (0.5 - 0.5 * rows))
        sq = xpos * xpos + ypos * ypos
        inv_s = lax.rsqrt(sq)
        cyl = sq * inv_s
        cosp = xpos * inv_s
        sinp = ypos * inv_s
        for p in range(depth):
            zpos = (s * depth + p).astype(jnp.float32) + (0.5 - 0.5 * slabs * depth)
            inv_r = lax.rsqrt(sq + zpos * zpos)
            zr = zpos * inv_r
            theta = (zr * cosp, zr * sinp, -(cyl * inv_r))
            phi = (-sinp, cosp)
            curv = []
            grad = []
            for h in range(6, 12):
                here, xs, ys, zs = near(h, r0, p)
                curv.append(here)
                grad.append((d12(*xs), d12(*ys), d12(*zs)))
            trace = curv[0] + curv[3] + curv[5]
            table = ((0, 1, 2), (1, 3, 4), (2, 4, 5))
            pairs = ((0, 0), (0, 1), (0, 2), (1, 1), (1, 2), (2, 2))

            def curl(i, j):
                n1, n2 = (i + 1) % 3, (i + 2) % 3
                return grad[table[n2][j]][n1] - grad[table[n1][j]][n2]

            real = None
            imag = None
            for at, (i, j) in enumerate(pairs):
                here, xs, ys, zs = near(at, r0, p)
                lap = lap_sum(xs, ys, zs) - 90.0 * here
                elec = lap * (-0.5 / 12.0) - trace * curv[at]
                for m in range(3):
                    elec = elec + curv[table[i][m]] * curv[table[m][j]]
                if i == j:
                    mag = curl(i, i) * (1.0 / 12.0)
                else:
                    mag = (curl(i, j) + curl(j, i)) * (0.5 / 12.0)
                fi = phi[i] if i < 2 else None
                fj = phi[j] if j < 2 else None
                tt = theta[i] * theta[j]
                both = tt if fi is None or fj is None else tt - fi * fj
                mixed = None
                for u, v in ((theta[i], fj), (theta[j], fi)):
                    if v is not None:
                        mixed = u * v if mixed is None else mixed + u * v
                if i == j:
                    both = 0.5 * both
                    mixed = None if mixed is None else 0.5 * mixed
                one = elec * both
                two = mag * both
                if mixed is not None:
                    one = one - mag * mixed
                    two = two + elec * mixed
                real = one if real is None else real + one
                imag = two if imag is None else imag + two
            imag = -imag
            per = ROWS // share
            for k in range(per):
                wl[tile * per + k, 0, p] = real[k * share:(k + 1) * share]
                wl[tile * per + k, 1, p] = imag[k * share:(k + 1) * share]

    def weyl_send(tile):
        per = ROWS // share
        for k in range(per):
            to = tile * per + k

            @pl.when(to == d)
            def _():
                pltpu.make_async_copy(
                    wl.at[to], weyl.at[:, pl.ds(d * depth, depth)], wlocal).start()

            @pl.when(to != d)
            def _():
                pltpu.make_async_remote_copy(
                    wl.at[to], weyl.at[:, pl.ds(d * depth, depth)], wsend, wrecv,
                    device_id={"dev": to}, device_id_type=MESH).start()

    def rhs_tile(tile):
        r0 = tile * ROWS
        mid = pl.ds(pl.multiple_of(r0 + 8, 8), ROWS)
        out = pl.ds(pl.multiple_of(r0, 8), ROWS)

        def stencil(h4, _):
            for p in range(depth):
                bz = own[12, p, mid, :] * (1.0 / 12.0)
                by = own[13, p, mid, :] * (1.0 / 12.0)
                bx = own[14, p, mid, :] * (1.0 / 12.0)
                for k in range(4):
                    h = h4 * 4 + k
                    here, xs, ys, zs = near(h, r0, p)
                    tsum[h, p] = lap_sum(xs, ys, zs)
                    rhs[h, p, out, :] = bx * d12(*xs) + by * d12(*ys) + bz * d12(*zs)
            return 0

        lax.fori_loop(0, F // 4, stencil, 0)
        for c0 in range(0, F, BLOCK):
            def mixing(h4, acc):
                for k in range(4):
                    h = h4 * 4 + k
                    acc = acc + w1[h, pl.ds(c0, BLOCK)][:, None] * own[h, :, mid, :][None]
                    acc = acc + w2[h, pl.ds(c0, BLOCK)][:, None] * tsum[h][None]
                return acc
            start = rhs[pl.ds(c0, BLOCK), :, out, :]
            rhs[pl.ds(c0, BLOCK), :, out, :] = lax.fori_loop(0, F // 4, mixing, start)

    def step(k, _):
        @pl.when(k < steps)
        def _():
            from_partner(k).wait_recv()

            @pl.when(relays)
            def _():
                relay(k).start()

        j = k - LAG

        @pl.when(j >= 0)
        def _():
            pltpu.make_async_remote_copy(
                own_chunk(j), halo_chunk(odd, j), send_r.at[j], recv_r.at[j],
                device_id={"dev": partner}, device_id_type=MESH).wait_recv()
            if WEYL:
                @pl.when((j >= 1) & (j <= tiles))
                def _():
                    weyl_send(j - 1)

            if COMPUTE:
                @pl.when(j < tiles)
                def _():
                    weyl_tile(j)

                @pl.when(j >= tiles)
                def _():
                    rhs_tile(j - tiles)
        return 0

    lax.fori_loop(0, steps + LAG, step, 0)

    def finish(k, _):
        to_partner(k).wait_send()

        @pl.when(relays)
        def _():
            relay(k).wait_send()

        @pl.when(direct)
        def _():
            straight(k).wait_send()
        return 0

    lax.fori_loop(0, steps, finish, 0)
    if WEYL:
        sent = wl.at[pl.ds(0, members - 1)]
        pltpu.make_async_copy(sent, sent, wsend).wait()
        came = weyl.at[:, pl.ds(0, depth * (members - 1))]
        pltpu.make_async_copy(came, came, wrecv).wait()
        pltpu.make_async_copy(wl.at[0], weyl.at[:, pl.ds(0, depth)], wlocal).wait()


def per_device(groups, members, fields, mix_matrix, laplace_matrix):
    depth, rows, width = fields.shape[1:]
    share = rows // members
    steps = 2 * (rows // ROWS)
    dma = pltpu.SemaphoreType.DMA
    return pl.pallas_call(
        functools.partial(kernel, groups, members),
        out_shape=(
            jax.ShapeDtypeStruct(fields.shape, jnp.float32),
            jax.ShapeDtypeStruct((2, depth * members, share, width), jnp.float32),
        ),
        in_specs=[
            pl.BlockSpec(memory_space=pltpu.HBM),
            pl.BlockSpec(memory_space=pltpu.SMEM),
            pl.BlockSpec(memory_space=pltpu.SMEM),
        ],
        out_specs=(pl.BlockSpec(memory_space=pltpu.VMEM), pl.BlockSpec(memory_space=pl.ANY)),
        scratch_shapes=[
            pltpu.VMEM((F, depth, rows + 16, width), jnp.float32),
            pltpu.VMEM((2, F, depth, rows, width), jnp.float32),
            pltpu.VMEM((F, depth, ROWS, width), jnp.float32),
            pltpu.VMEM((F, F, 8, 128), jnp.float32),
            pltpu.VMEM((F, F, 8, 128), jnp.float32),
            pltpu.VMEM((members, 2, depth, share, width), jnp.float32),
            dma((4,)), dma((steps,)), dma((steps,)), dma((steps,)), dma((steps,)), dma((steps,)),
            dma, dma, dma,
        ],
        compiler_params=pltpu.CompilerParams(
            collective_id=0, has_side_effects=True, vmem_limit_bytes=40 * 1024 * 1024
        ),
    )(fields, mix_matrix, laplace_matrix)


def solution(mesh):
    groups, members = mesh.shape["grp"], mesh.shape["dev"]
    return jax.shard_map(
        functools.partial(per_device, groups, members),
        mesh=mesh,
        in_specs=(P(None, ("grp", "dev"), None, None), P(), P()),
        out_specs=(P(None, ("grp", "dev"), None, None), P(None, "grp", "dev", None)),
        check_vma=False,
    )
```

```python
import functools

import jax
import jax.numpy as jnp
from jax import lax
from jax.experimental import pallas as pl
from jax.experimental.pallas import tpu as pltpu
from jax.sharding import PartitionSpec as P

MESH = pl.DeviceIdType.MESH
F = 24
HALF = 12
ROWS = 8
LAG = 8
SUB = 1
BLOCK = 12
COMPUTE = True
WEYL = True


def d12(m2, m1, p1, p2):
    return 8.0 * (p1 - m1) - (p2 - m2)


def kernel(groups, members, fields, mix_in, lap_in, rhs, weyl, own, halo, tsum, w1, w2, wl,
           mix, lapw, wrow, load_sem, send_p, recv_p, send_r, recv_r, send_d, wsend, wrecv, wlocal):
    depth = fields.shape[1]
    rows = fields.shape[2]
    width = fields.shape[3]
    tiles = rows // ROWS
    steps = 2 * tiles
    width_f = HALF // SUB
    share = rows // members
    g = lax.axis_index("grp")
    d = lax.axis_index("dev")
    slabs = groups * members
    s = g * members + d
    odd = lax.rem(d, 2)
    partner = d + 1 - 2 * odd
    target = lax.rem(s + 2 - 4 * odd + slabs, slabs)
    target_id = {"grp": target // members, "dev": lax.rem(target, members)}
    nearby = lax.rem(s - 1 + 2 * odd + slabs, slabs)
    nearby_id = {"grp": nearby // members, "dev": lax.rem(nearby, members)}
    godd = lax.rem(g, 2)
    last = d >= members - 2
    first = d < 2
    cross = (last & (godd == 1)) | (first & (godd == 0))
    relays = jnp.logical_not(cross & ((d == members - 2) | (d == 1)))
    direct = cross & ((d == members - 1) | (d == 0))

    loads = []
    for half in range(2):
        part = pl.ds(half * HALF, HALF)
        loads.append(pltpu.make_async_copy(
            fields.at[part], own.at[part, :, pl.ds(8, rows), :], load_sem.at[half]))
    loads.append(pltpu.make_async_copy(
        fields.at[:, :, pl.ds(rows - 8, 8), :], own.at[:, :, pl.ds(0, 8), :], load_sem.at[2]))
    loads.append(pltpu.make_async_copy(
        fields.at[:, :, pl.ds(0, 8), :], own.at[:, :, pl.ds(rows + 8, 8), :], load_sem.at[3]))
    loads.append(pltpu.make_async_copy(mix_in, mix, load_sem.at[4]))
    loads.append(pltpu.make_async_copy(lap_in, lapw, load_sem.at[5]))
    for load in loads:
        load.start()

    barrier = pltpu.get_barrier_semaphore()

    def greet(offset, _):
        pl.semaphore_signal(barrier, inc=1, device_id={"dev": lax.rem(d + offset, members)},
                            device_id_type=MESH)
        return 0

    lax.fori_loop(1, members, greet, 0)
    edge = jnp.where(last, 1, jnp.where(first, 1, 0))

    @pl.when(edge == 1)
    def _():
        other = lax.rem(g + jnp.where(last, 1, groups - 1), groups)
        base = jnp.where(last, 0, members - 2)
        for k in range(2):
            pl.semaphore_signal(barrier, inc=1, device_id={"grp": other, "dev": base + k},
                                device_id_type=MESH)

    pl.semaphore_wait(barrier, members - 1 + 2 * edge)

    def window(k):
        part, sub = k // SUB, lax.rem(k, SUB)
        return (part // tiles) * HALF + sub * width_f, lax.rem(part, tiles) * ROWS

    def own_chunk(k):
        f0, r0 = window(k)
        return own.at[pl.ds(f0, width_f), :, pl.ds(pl.multiple_of(r0 + 8, 8), ROWS), :]

    def halo_chunk(slot, k):
        f0, r0 = window(k)
        return halo.at[slot, pl.ds(f0, width_f), :, pl.ds(pl.multiple_of(r0, 8), ROWS), :]

    mine = 1 - odd

    def to_partner(k):
        return pltpu.make_async_remote_copy(
            own_chunk(k), halo_chunk(odd, k), send_p.at[k], recv_p.at[k],
            device_id={"dev": partner}, device_id_type=MESH)

    def from_partner(k):
        return pltpu.make_async_remote_copy(
            own_chunk(k), halo_chunk(mine, k), send_p.at[k], recv_p.at[k],
            device_id={"dev": partner}, device_id_type=MESH)

    def relay(k):
        return pltpu.make_async_remote_copy(
            halo_chunk(mine, k), halo_chunk(odd, k), send_r.at[k], recv_r.at[k],
            device_id=target_id, device_id_type=MESH)

    def straight(k):
        return pltpu.make_async_remote_copy(
            own_chunk(k), halo_chunk(mine, k), send_d.at[k], recv_r.at[k],
            device_id=nearby_id, device_id_type=MESH)

    def first_sends(k, _):
        to_partner(k).start()
        return 0

    loads[0].wait()
    lax.fori_loop(0, tiles * SUB, first_sends, 0)
    loads[1].wait()
    lax.fori_loop(tiles * SUB, steps * SUB, first_sends, 0)
    loads[2].wait()
    loads[3].wait()

    loads[4].wait()
    loads[5].wait()
    if COMPUTE:
        lap_all = lapw[...]
        for at, table in enumerate((mix[...] - 7.5 * lap_all, lap_all * (1.0 / 12.0))):
            for h in range(F):
                wrow[at, h] = jnp.broadcast_to(table[:, h:h + 1], (F, 128))

        def spread(h, _):
            for at, into in enumerate((w1, w2)):
                for c in range(F):
                    into[h, c] = jnp.broadcast_to(wrow[at, h, c:c + 1, :], (8, 128))
            return 0

        lax.fori_loop(0, F, spread, 0)

    lane = lax.broadcasted_iota(jnp.int32, (ROWS, width), 1).astype(jnp.float32)
    line = lax.broadcasted_iota(jnp.int32, (ROWS, width), 0).astype(jnp.float32)

    def near(h, r0, p, halos=True):
        def at(off):
            return own[h, p, pl.ds(r0 + 8 + off, ROWS), :]
        mid = pl.ds(pl.multiple_of(r0 + 8, 8), ROWS)
        here = own[h, p, mid, :]
        rows_at = pl.ds(pl.multiple_of(r0, 8), ROWS)
        xs = [pltpu.roll(here, 2, 1), pltpu.roll(here, 1, 1),
              pltpu.roll(here, width - 1, 1), pltpu.roll(here, width - 2, 1)]
        ys = [at(-2), at(-1), at(1), at(2)]
        other = own[h, 1 - p, mid, :]
        if not halos:
            return here, xs, ys, other
        if p == 0:
            zs = [halo[0, h, 0, rows_at, :], halo[0, h, 1, rows_at, :],
                  other, halo[1, h, 0, rows_at, :]]
        else:
            zs = [halo[0, h, 1, rows_at, :], other,
                  halo[1, h, 0, rows_at, :], halo[1, h, 1, rows_at, :]]
        return here, xs, ys, zs

    def lap_sum(xs, ys, zs):
        one = (xs[1] + xs[2]) + (ys[1] + ys[2]) + (zs[1] + zs[2])
        two = (xs[0] + xs[3]) + (ys[0] + ys[3]) + (zs[0] + zs[3])
        return 16.0 * one - two

    def weyl_tile(tile):
        r0 = tile * ROWS
        xpos = lane + (0.5 - 0.5 * width)
        ypos = line + (r0.astype(jnp.float32) + (0.5 - 0.5 * rows))
        sq = xpos * xpos + ypos * ypos
        inv_s = lax.rsqrt(sq)
        cyl = sq * inv_s
        cosp = xpos * inv_s
        sinp = ypos * inv_s
        for p in range(depth):
            zpos = (s * depth + p).astype(jnp.float32) + (0.5 - 0.5 * slabs * depth)
            inv_r = lax.rsqrt(sq + zpos * zpos)
            zr = zpos * inv_r
            theta = (zr * cosp, zr * sinp, -(cyl * inv_r))
            phi = (-sinp, cosp)
            curv = []
            grad = []
            for h in range(6, 12):
                here, xs, ys, zs = near(h, r0, p)
                curv.append(here)
                grad.append((d12(*xs), d12(*ys), d12(*zs)))
            trace = curv[0] + curv[3] + curv[5]
            table = ((0, 1, 2), (1, 3, 4), (2, 4, 5))
            pairs = ((0, 0), (0, 1), (0, 2), (1, 1), (1, 2), (2, 2))

            def curl(i, j):
                n1, n2 = (i + 1) % 3, (i + 2) % 3
                return grad[table[n2][j]][n1] - grad[table[n1][j]][n2]

            real = None
            imag = None
            for at, (i, j) in enumerate(pairs):
                here, xs, ys, zs = near(at, r0, p)
                lap = lap_sum(xs, ys, zs) - 90.0 * here
                elec = lap * (-0.5 / 12.0) - trace * curv[at]
                for m in range(3):
                    elec = elec + curv[table[i][m]] * curv[table[m][j]]
                if i == j:
                    mag = curl(i, i) * (1.0 / 12.0)
                else:
                    mag = (curl(i, j) + curl(j, i)) * (0.5 / 12.0)
                fi = phi[i] if i < 2 else None
                fj = phi[j] if j < 2 else None
                tt = theta[i] * theta[j]
                both = tt if fi is None or fj is None else tt - fi * fj
                mixed = None
                for u, v in ((theta[i], fj), (theta[j], fi)):
                    if v is not None:
                        mixed = u * v if mixed is None else mixed + u * v
                if i == j:
                    both = 0.5 * both
                    mixed = None if mixed is None else 0.5 * mixed
                one = elec * both
                two = mag * both
                if mixed is not None:
                    one = one - mag * mixed
                    two = two + elec * mixed
                real = one if real is None else real + one
                imag = two if imag is None else imag + two
            imag = -imag
            per = ROWS // share
            for k in range(per):
                wl[tile * per + k, 0, p] = real[k * share:(k + 1) * share]
                wl[tile * per + k, 1, p] = imag[k * share:(k + 1) * share]

    def weyl_send(tile):
        per = ROWS // share
        for k in range(per):
            to = tile * per + k

            @pl.when(to == d)
            def _():
                pltpu.make_async_copy(
                    wl.at[to], weyl.at[:, pl.ds(d * depth, depth)], wlocal).start()

            @pl.when(to != d)
            def _():
                pltpu.make_async_remote_copy(
                    wl.at[to], weyl.at[:, pl.ds(d * depth, depth)], wsend, wrecv,
                    device_id={"dev": to}, device_id_type=MESH).start()

    def mixed(tile, h0, h1, with_own):
        mid = pl.ds(pl.multiple_of(tile * ROWS + 8, 8), ROWS)
        out = pl.ds(pl.multiple_of(tile * ROWS, 8), ROWS)
        for c0 in range(0, F, BLOCK):
            def mixing(h4, acc):
                for k in range(4):
                    h = h4 * 4 + k
                    if with_own:
                        acc = acc + w1[h, pl.ds(c0, BLOCK)][:, None] * own[h, :, mid, :][None]
                    acc = acc + w2[h, pl.ds(c0, BLOCK)][:, None] * tsum[h][None]
                return acc
            start = rhs[pl.ds(c0, BLOCK), :, out, :]
            rhs[pl.ds(c0, BLOCK), :, out, :] = lax.fori_loop(h0 // 4, h1 // 4, mixing, start)

    def rhs_early(tile):
        r0 = tile * ROWS
        mid = pl.ds(pl.multiple_of(r0 + 8, 8), ROWS)
        out = pl.ds(pl.multiple_of(r0, 8), ROWS)

        def stencil(halos, h4, _):
            for p in range(depth):
                bz = own[12, p, mid, :] * (1.0 / 12.0)
                by = own[13, p, mid, :] * (1.0 / 12.0)
                bx = own[14, p, mid, :] * (1.0 / 12.0)
                for k in range(4):
                    h = h4 * 4 + k
                    here, xs, ys, zs = near(h, r0, p, halos)
                    if halos:
                        tsum[h, p] = lap_sum(xs, ys, zs)
                        dz = d12(*zs)
                    else:
                        one = (xs[1] + xs[2]) + (ys[1] + ys[2]) + zs
                        two = (xs[0] + xs[3]) + (ys[0] + ys[3])
                        tsum[h, p] = 16.0 * one - two
                        dz = (8.0 if p == 0 else -8.0) * zs
                    rhs[h, p, out, :] = bx * d12(*xs) + by * d12(*ys) + bz * dz
            return 0

        lax.fori_loop(0, HALF // 4, functools.partial(stencil, True), 0)
        lax.fori_loop(HALF // 4, F // 4, functools.partial(stencil, False), 0)
        mixed(tile, 0, F, True)

    def rhs_late(tile):
        r0 = tile * ROWS
        mid = pl.ds(pl.multiple_of(r0 + 8, 8), ROWS)
        out = pl.ds(pl.multiple_of(r0, 8), ROWS)

        def planes(h4, _):
            for p in range(depth):
                bz = own[12, p, mid, :] * (1.0 / 12.0)
                for k in range(4):
                    h = h4 * 4 + k
                    below = halo[0, h, 1, out, :]
                    above = halo[1, h, 0, out, :]
                    if p == 0:
                        far = halo[0, h, 0, out, :]
                        tsum[h, p] = 16.0 * below - (far + above)
                        dz = (far - above) - 8.0 * below
                    else:
                        far = halo[1, h, 1, out, :]
                        tsum[h, p] = 16.0 * above - (below + far)
                        dz = 8.0 * above + (below - far)
                    rhs[h, p, out, :] = rhs[h, p, out, :] + bz * dz
            return 0

        lax.fori_loop(HALF // 4, F // 4, planes, 0)
        mixed(tile, HALF, F, False)

    def relay_step(k, _):
        from_partner(k).wait_recv()

        @pl.when(relays)
        def _():
            relay(k).start()

        @pl.when(direct)
        def _():
            straight(k).start()
        return 0

    def relayed(k, _):
        pltpu.make_async_remote_copy(
            own_chunk(k), halo_chunk(odd, k), send_r.at[k], recv_r.at[k],
            device_id={"dev": partner}, device_id_type=MESH).wait_recv()
        return 0

    def step(part, _):
        @pl.when(part < steps)
        def _():
            lax.fori_loop(part * SUB, part * SUB + SUB, relay_step, 0)

        j = part - LAG

        @pl.when(j >= 0)
        def _():
            lax.fori_loop(j * SUB, j * SUB + SUB, relayed, 0)
            if WEYL:
                @pl.when((j >= 1) & (j <= tiles))
                def _():
                    weyl_send(j - 1)

            if COMPUTE:
                @pl.when(j < tiles)
                def _():
                    weyl_tile(j)
                    rhs_early(j)

                @pl.when(j >= tiles)
                def _():
                    rhs_late(j - tiles)
        return 0

    lax.fori_loop(0, steps + LAG, step, 0)

    def finish(k, _):
        to_partner(k).wait_send()

        @pl.when(relays)
        def _():
            relay(k).wait_send()

        @pl.when(direct)
        def _():
            straight(k).wait_send()
        return 0

    lax.fori_loop(0, steps * SUB, finish, 0)
    if WEYL:
        sent = wl.at[pl.ds(0, members - 1)]
        pltpu.make_async_copy(sent, sent, wsend).wait()
        came = weyl.at[:, pl.ds(0, depth * (members - 1))]
        pltpu.make_async_copy(came, came, wrecv).wait()
        pltpu.make_async_copy(wl.at[0], weyl.at[:, pl.ds(0, depth)], wlocal).wait()


def per_device(groups, members, fields, mix_matrix, laplace_matrix):
    depth, rows, width = fields.shape[1:]
    share = rows // members
    chunks = 2 * (rows // ROWS) * SUB
    arrays = [pltpu.with_memory_space_constraint(a, pltpu.HBM)
              for a in (fields, mix_matrix, laplace_matrix)]
    dma = pltpu.SemaphoreType.DMA
    return pl.pallas_call(
        functools.partial(kernel, groups, members),
        out_shape=(
            jax.ShapeDtypeStruct(fields.shape, jnp.float32),
            jax.ShapeDtypeStruct((2, depth * members, share, width), jnp.float32),
        ),
        in_specs=[
            pl.BlockSpec(memory_space=pltpu.HBM),
            pl.BlockSpec(memory_space=pltpu.HBM),
            pl.BlockSpec(memory_space=pltpu.HBM),
        ],
        out_specs=(pl.BlockSpec(memory_space=pltpu.VMEM), pl.BlockSpec(memory_space=pl.ANY)),
        scratch_shapes=[
            pltpu.VMEM((F, depth, rows + 16, width), jnp.float32),
            pltpu.VMEM((2, F, depth, rows, width), jnp.float32),
            pltpu.VMEM((F, depth, ROWS, width), jnp.float32),
            pltpu.VMEM((F, F, 8, 128), jnp.float32),
            pltpu.VMEM((F, F, 8, 128), jnp.float32),
            pltpu.VMEM((members, 2, depth, share, width), jnp.float32),
            pltpu.VMEM((F, F), jnp.float32),
            pltpu.VMEM((F, F), jnp.float32),
            pltpu.VMEM((2, F, F, 128), jnp.float32),
            dma((6,)), dma((chunks,)), dma((chunks,)), dma((chunks,)), dma((chunks,)), dma((chunks,)),
            dma, dma, dma,
        ],
        compiler_params=pltpu.CompilerParams(
            collective_id=0, has_side_effects=True, vmem_limit_bytes=40 * 1024 * 1024
        ),
    )(*arrays)


def solution(mesh):
    groups, members = mesh.shape["grp"], mesh.shape["dev"]
    return jax.shard_map(
        functools.partial(per_device, groups, members),
        mesh=mesh,
        in_specs=(P(None, ("grp", "dev"), None, None), P(), P()),
        out_specs=(P(None, ("grp", "dev"), None, None), P(None, "grp", "dev", None)),
        check_vma=False,
    )
```

```python
import functools

import jax
import jax.numpy as jnp
from jax import lax
from jax.experimental import pallas as pl
from jax.experimental.pallas import tpu as pltpu
from jax.sharding import PartitionSpec as P

MESH = pl.DeviceIdType.MESH
F = 24
HALF = 12
ROWS = 8
LAG = 8
TAIL = 4
HOLD_P = 3
HOLD_R = 2
HOLD_D = 4
HOLD_V = 5
BLOCK = 12
COMPUTE = True
WEYL = True


def d12(m2, m1, p1, p2):
    return 8.0 * (p1 - m1) - (p2 - m2)


def kernel(groups, members, fields, mix_in, lap_in, rhs, weyl, own, halo, via, tsum, w1, w2, wl,
           mix, lapw, wrow, load_sem, send_p, recv_p, send_r, recv_r, send_d, recv_d, wsend, wrecv, wlocal,
           up, far, ready):
    depth = fields.shape[1]
    rows = fields.shape[2]
    width = fields.shape[3]
    tiles = rows // ROWS
    steps = 2 * tiles
    share = rows // members
    g = lax.axis_index("grp")
    d = lax.axis_index("dev")
    slabs = groups * members
    s = g * members + d
    odd = lax.rem(d, 2)
    partner = d + 1 - 2 * odd
    target = lax.rem(s + 2 - 4 * odd + slabs, slabs)
    target_id = {"grp": target // members, "dev": lax.rem(target, members)}
    end = members - 1
    godd = lax.rem(g, 2)

    def group(by):
        return {"grp": lax.rem(g + by + groups, groups)}

    hub = ((godd == 1) & (d == end - 1)) | ((godd == 0) & (d == 1))
    direct = ((godd == 1) & (d == end)) | ((godd == 0) & (d == 0))
    relays = jnp.logical_not(hub)
    hub_id = {"grp": lax.rem(g + 1 - 2 * godd + groups, groups), "dev": jnp.where(d == 0, end - 1, 1)}
    hub_target = {**group(2), "dev": jnp.where(d == 1, 0, end)}

    loads = []
    for half in range(2):
        part = pl.ds(half * HALF, HALF)
        loads.append(pltpu.make_async_copy(
            fields.at[part], own.at[part, :, pl.ds(8, rows), :], load_sem.at[half]))
    loads.append(pltpu.make_async_copy(
        fields.at[:, :, pl.ds(rows - 8, 8), :], own.at[:, :, pl.ds(0, 8), :], load_sem.at[2]))
    loads.append(pltpu.make_async_copy(
        fields.at[:, :, pl.ds(0, 8), :], own.at[:, :, pl.ds(rows + 8, 8), :], load_sem.at[3]))
    loads.append(pltpu.make_async_copy(mix_in, mix, load_sem.at[4]))
    loads.append(pltpu.make_async_copy(lap_in, lapw, load_sem.at[5]))
    for load in loads:
        load.start()

    barrier = pltpu.get_barrier_semaphore()

    def hello(to):
        pl.semaphore_signal(barrier, inc=1, device_id=to, device_id_type=MESH)

    def greet(to, _):
        hello({"dev": to})
        return 0

    @pl.when(odd == 1)
    def _():
        hello({"dev": d - 1})

    lax.fori_loop(d + 1, members, greet, 0)

    @pl.when((d == 0) & (godd == 1))
    def _():
        hello({**group(-1), "dev": end - 1})

    @pl.when((d == 1) & (godd == 1))
    def _():
        hello({**group(-1), "dev": end})

    @pl.when((d == 0) & (godd == 0))
    def _():
        hello({**group(1), "dev": end - 1})
        hello({**group(2), "dev": 1})

    @pl.when((d == 1) & (godd == 0))
    def _():
        hello({**group(1), "dev": end})

    @pl.when((d == end) & (godd == 1))
    def _():
        hello({**group(2), "dev": end - 1})

    extra = jnp.where(d == end, 1, jnp.where(d == end - 1, 1 + godd, jnp.where(d == 1, 1 - godd, 0)))
    pl.semaphore_wait(barrier, d + (1 - odd) + extra)

    big = steps - 1

    def window(k, tail):
        if tail:
            size = HALF // TAIL
            return pl.ds(HALF + (k - big) * size, size), rows - ROWS
        return pl.ds((k // tiles) * HALF, HALF), pl.multiple_of(lax.rem(k, tiles) * ROWS, ROWS)

    def each(body, head=True, tail=True):
        def run(is_tail, k, _):
            body(k, is_tail)
            return 0
        if head:
            lax.fori_loop(0, big, functools.partial(run, False), 0)
        if tail:
            lax.fori_loop(big, big + TAIL, functools.partial(run, True), 0)

    def own_chunk(k, tail):
        part, r0 = window(k, tail)
        return own.at[part, :, pl.ds(r0 + 8, ROWS), :]

    def halo_chunk(slot, k, tail):
        part, r0 = window(k, tail)
        return halo.at[slot, part, :, pl.ds(r0, ROWS), :]

    def via_chunk(k, tail):
        part, r0 = window(k, tail)
        return via.at[part, :, pl.ds(r0, ROWS), :]

    mine = 1 - odd

    def to_partner(k, tail):
        return pltpu.make_async_remote_copy(
            own_chunk(k, tail), halo_chunk(odd, k, tail), send_p.at[k], recv_p.at[k],
            device_id={"dev": partner}, device_id_type=MESH)

    def relay(k, tail):
        return pltpu.make_async_remote_copy(
            halo_chunk(mine, k, tail), halo_chunk(odd, k, tail), send_r.at[k], recv_r.at[k],
            device_id=target_id, device_id_type=MESH)

    def straight(k, tail):
        return pltpu.make_async_remote_copy(
            own_chunk(k, tail), via_chunk(k, tail), send_d.at[k], recv_d.at[k],
            device_id=hub_id, device_id_type=MESH)

    def hand_on(k, tail):
        return pltpu.make_async_remote_copy(
            via_chunk(k, tail), halo_chunk(mine, k, tail), send_r.at[k], recv_r.at[k],
            device_id=hub_target, device_id_type=MESH)

    def send(k, tail):
        to_partner(k, tail).start()

    def send_straight(k, tail):
        straight(k, tail).start()

    yields = (d == end) & (godd == 1)

    def send_half(half):
        def run(k, _):
            send(k, False)
            return 0

        @pl.when(jnp.logical_not(yields))
        def _():
            lax.fori_loop(half * tiles, tiles if half == 0 else big, run, 0)

    loads[0].wait()
    send_half(0)

    @pl.when((odd == 0) & (d >= 2))
    def _():
        pl.semaphore_signal(up, inc=1, device_id={"dev": d - 2}, device_id_type=MESH)

    @pl.when((d == end) & (godd == 0))
    def _():
        pl.semaphore_signal(up, inc=1, device_id={**group(1), "dev": 1}, device_id_type=MESH)

    @pl.when((d == end - 1) & (godd == 1))
    def _():
        pl.semaphore_signal(far, inc=1, device_id={**group(-1), "dev": 0}, device_id_type=MESH)

    loads[1].wait()
    send_half(1)

    @pl.when(jnp.logical_not(yields))
    def _():
        each(send, head=False)

    @pl.when(yields)
    def _():
        each(send_straight)

    def reply(to, _):
        pl.semaphore_signal(ready, inc=1, device_id={"dev": to}, device_id_type=MESH)
        return 0

    lax.fori_loop(0, d, reply, 0)
    loads[2].wait()
    loads[3].wait()

    loads[4].wait()
    loads[5].wait()
    if COMPUTE:
        lap_all = lapw[...]
        for at, table in enumerate((mix[...] - 7.5 * lap_all, lap_all * (1.0 / 12.0))):
            for h in range(F):
                wrow[at, h] = jnp.broadcast_to(table[:, h:h + 1], (F, 128))

        def spread(h, _):
            for at, into in enumerate((w1, w2)):
                for c in range(F):
                    into[h, c] = jnp.broadcast_to(wrow[at, h, c:c + 1, :], (8, 128))
            return 0

        lax.fori_loop(0, F, spread, 0)

    lane = lax.broadcasted_iota(jnp.int32, (ROWS, width), 1).astype(jnp.float32)
    line = lax.broadcasted_iota(jnp.int32, (ROWS, width), 0).astype(jnp.float32)

    def near(h, r0, p, halos=True):
        def at(off):
            return own[h, p, pl.ds(r0 + 8 + off, ROWS), :]
        mid = pl.ds(pl.multiple_of(r0 + 8, 8), ROWS)
        here = own[h, p, mid, :]
        rows_at = pl.ds(pl.multiple_of(r0, 8), ROWS)
        xs = [pltpu.roll(here, 2, 1), pltpu.roll(here, 1, 1),
              pltpu.roll(here, width - 1, 1), pltpu.roll(here, width - 2, 1)]
        ys = [at(-2), at(-1), at(1), at(2)]
        other = own[h, 1 - p, mid, :]
        if not halos:
            return here, xs, ys, other
        if p == 0:
            zs = [halo[0, h, 0, rows_at, :], halo[0, h, 1, rows_at, :],
                  other, halo[1, h, 0, rows_at, :]]
        else:
            zs = [halo[0, h, 1, rows_at, :], other,
                  halo[1, h, 0, rows_at, :], halo[1, h, 1, rows_at, :]]
        return here, xs, ys, zs

    def lap_sum(xs, ys, zs):
        one = (xs[1] + xs[2]) + (ys[1] + ys[2]) + (zs[1] + zs[2])
        two = (xs[0] + xs[3]) + (ys[0] + ys[3]) + (zs[0] + zs[3])
        return 16.0 * one - two

    def weyl_tile(tile):
        r0 = tile * ROWS
        xpos = lane + (0.5 - 0.5 * width)
        ypos = line + (r0.astype(jnp.float32) + (0.5 - 0.5 * rows))
        sq = xpos * xpos + ypos * ypos
        inv_s = lax.rsqrt(sq)
        cyl = sq * inv_s
        cosp = xpos * inv_s
        sinp = ypos * inv_s
        for p in range(depth):
            zpos = (s * depth + p).astype(jnp.float32) + (0.5 - 0.5 * slabs * depth)
            inv_r = lax.rsqrt(sq + zpos * zpos)
            zr = zpos * inv_r
            theta = (zr * cosp, zr * sinp, -(cyl * inv_r))
            phi = (-sinp, cosp)
            curv = []
            grad = []
            for h in range(6, 12):
                here, xs, ys, zs = near(h, r0, p)
                curv.append(here)
                grad.append((d12(*xs), d12(*ys), d12(*zs)))
            trace = curv[0] + curv[3] + curv[5]
            table = ((0, 1, 2), (1, 3, 4), (2, 4, 5))
            pairs = ((0, 0), (0, 1), (0, 2), (1, 1), (1, 2), (2, 2))

            def curl(i, j):
                n1, n2 = (i + 1) % 3, (i + 2) % 3
                return grad[table[n2][j]][n1] - grad[table[n1][j]][n2]

            real = None
            imag = None
            for at, (i, j) in enumerate(pairs):
                here, xs, ys, zs = near(at, r0, p)
                lap = lap_sum(xs, ys, zs) - 90.0 * here
                elec = lap * (-0.5 / 12.0) - trace * curv[at]
                for m in range(3):
                    elec = elec + curv[table[i][m]] * curv[table[m][j]]
                if i == j:
                    mag = curl(i, i) * (1.0 / 12.0)
                else:
                    mag = (curl(i, j) + curl(j, i)) * (0.5 / 12.0)
                fi = phi[i] if i < 2 else None
                fj = phi[j] if j < 2 else None
                tt = theta[i] * theta[j]
                both = tt if fi is None or fj is None else tt - fi * fj
                mixed = None
                for u, v in ((theta[i], fj), (theta[j], fi)):
                    if v is not None:
                        mixed = u * v if mixed is None else mixed + u * v
                if i == j:
                    both = 0.5 * both
                    mixed = None if mixed is None else 0.5 * mixed
                one = elec * both
                two = mag * both
                if mixed is not None:
                    one = one - mag * mixed
                    two = two + elec * mixed
                real = one if real is None else real + one
                imag = two if imag is None else imag + two
            imag = -imag
            per = ROWS // share
            for k in range(per):
                wl[tile * per + k, 0, p] = real[k * share:(k + 1) * share]
                wl[tile * per + k, 1, p] = imag[k * share:(k + 1) * share]

    def weyl_send(tile):
        per = ROWS // share
        for k in range(per):
            to = tile * per + k

            @pl.when(to == d)
            def _():
                pltpu.make_async_copy(
                    wl.at[to], weyl.at[:, pl.ds(d * depth, depth)], wlocal).start()

            @pl.when(to != d)
            def _():
                pltpu.make_async_remote_copy(
                    wl.at[to], weyl.at[:, pl.ds(d * depth, depth)], wsend, wrecv,
                    device_id={"dev": to}, device_id_type=MESH).start()

    def mixed(tile, h0, h1, with_own):
        mid = pl.ds(pl.multiple_of(tile * ROWS + 8, 8), ROWS)
        out = pl.ds(pl.multiple_of(tile * ROWS, 8), ROWS)
        for c0 in range(0, F, BLOCK):
            def mixing(h4, acc):
                for k in range(4):
                    h = h4 * 4 + k
                    if with_own:
                        acc = acc + w1[h, pl.ds(c0, BLOCK)][:, None] * own[h, :, mid, :][None]
                    acc = acc + w2[h, pl.ds(c0, BLOCK)][:, None] * tsum[h][None]
                return acc
            start = rhs[pl.ds(c0, BLOCK), :, out, :]
            rhs[pl.ds(c0, BLOCK), :, out, :] = lax.fori_loop(h0 // 4, h1 // 4, mixing, start)

    def rhs_early(tile):
        r0 = tile * ROWS
        mid = pl.ds(pl.multiple_of(r0 + 8, 8), ROWS)
        out = pl.ds(pl.multiple_of(r0, 8), ROWS)

        def stencil(halos, h4, _):
            for p in range(depth):
                bz = own[12, p, mid, :] * (1.0 / 12.0)
                by = own[13, p, mid, :] * (1.0 / 12.0)
                bx = own[14, p, mid, :] * (1.0 / 12.0)
                for k in range(4):
                    h = h4 * 4 + k
                    here, xs, ys, zs = near(h, r0, p, halos)
                    if halos:
                        tsum[h, p] = lap_sum(xs, ys, zs)
                        dz = d12(*zs)
                    else:
                        one = (xs[1] + xs[2]) + (ys[1] + ys[2]) + zs
                        two = (xs[0] + xs[3]) + (ys[0] + ys[3])
                        tsum[h, p] = 16.0 * one - two
                        dz = (8.0 if p == 0 else -8.0) * zs
                    rhs[h, p, out, :] = bx * d12(*xs) + by * d12(*ys) + bz * dz
            return 0

        lax.fori_loop(0, HALF // 4, functools.partial(stencil, True), 0)
        lax.fori_loop(HALF // 4, F // 4, functools.partial(stencil, False), 0)
        mixed(tile, 0, F, True)

    def rhs_late(tile):
        r0 = tile * ROWS
        mid = pl.ds(pl.multiple_of(r0 + 8, 8), ROWS)
        out = pl.ds(pl.multiple_of(r0, 8), ROWS)

        def planes(h4, _):
            for p in range(depth):
                bz = own[12, p, mid, :] * (1.0 / 12.0)
                for k in range(4):
                    h = h4 * 4 + k
                    below = halo[0, h, 1, out, :]
                    above = halo[1, h, 0, out, :]
                    if p == 0:
                        far = halo[0, h, 0, out, :]
                        tsum[h, p] = 16.0 * below - (far + above)
                        dz = (far - above) - 8.0 * below
                    else:
                        far = halo[1, h, 1, out, :]
                        tsum[h, p] = 16.0 * above - (below + far)
                        dz = 8.0 * above + (below - far)
                    rhs[h, p, out, :] = rhs[h, p, out, :] + bz * dz
            return 0

        lax.fori_loop(HALF // 4, F // 4, planes, 0)
        mixed(tile, HALF, F, False)

    asks = ((odd == 0) & (d < end - 1)) | ((d == 1) & (godd == 1))
    hold_relay = jnp.where((d == 1) & (godd == 1), HOLD_R, 0)
    hold_hub = jnp.where(d == 1, HOLD_V, 1)

    def arrived(k, tail):
        to_partner(k, tail).wait_recv()

    def relayed(k, tail):
        relay(k, tail).wait_recv()

    def pass_on(k, tail):
        straight(k, tail).wait_recv()
        hand_on(k, tail).start()

    def last_relay(k, tail):
        arrived(k, tail)

        @pl.when(relays)
        def _():
            relay(k, tail).start()

    def step(part, _):
        @pl.when(part < big)
        def _():
            arrived(part, False)

        @pl.when(yields & (part == HOLD_P))
        def _():
            each(send)

        @pl.when(direct & (d == 0) & (part == HOLD_D))
        def _():
            pl.semaphore_wait(far, 1)
            each(send_straight)

        r = part - hold_relay

        @pl.when(relays & (r >= 0) & (r < big))
        def _():
            @pl.when(asks & (r == 0))
            def _():
                pl.semaphore_wait(up, 1)
            relay(r, False).start()

        @pl.when(r == big)
        def _():
            each(last_relay, head=False)

        v = part - hold_hub

        @pl.when(hub & (v >= 0) & (v < big))
        def _():
            pass_on(v, False)

        @pl.when(hub & (v == big))
        def _():
            each(pass_on, head=False)

        j = part - LAG

        @pl.when((j >= 0) & (j < big))
        def _():
            relayed(j, False)

        @pl.when(j == big)
        def _():
            each(relayed, head=False)

        if WEYL:
            @pl.when((j == 1) & (d < end))
            def _():
                pl.semaphore_wait(ready, end - d)

            @pl.when((j >= 1) & (j <= tiles))
            def _():
                weyl_send(j - 1)

        if COMPUTE:
            @pl.when((j >= 0) & (j < tiles))
            def _():
                weyl_tile(j)
                rhs_early(j)

            @pl.when(j >= tiles)
            def _():
                rhs_late(j - tiles)
        return 0

    lax.fori_loop(0, steps + LAG, step, 0)

    def sent_all(k, tail):
        to_partner(k, tail).wait_send()
        relay(k, tail).wait_send()

        @pl.when(direct)
        def _():
            straight(k, tail).wait_send()

    each(sent_all)
    if WEYL:
        sent = wl.at[pl.ds(0, members - 1)]
        pltpu.make_async_copy(sent, sent, wsend).wait()
        came = weyl.at[:, pl.ds(0, depth * (members - 1))]
        pltpu.make_async_copy(came, came, wrecv).wait()
        pltpu.make_async_copy(wl.at[0], weyl.at[:, pl.ds(0, depth)], wlocal).wait()


def per_device(groups, members, fields, mix_matrix, laplace_matrix):
    depth, rows, width = fields.shape[1:]
    share = rows // members
    chunks = 2 * (rows // ROWS) - 1 + TAIL
    arrays = [pltpu.with_memory_space_constraint(a, pltpu.HBM)
              for a in (fields, mix_matrix, laplace_matrix)]
    dma = pltpu.SemaphoreType.DMA
    regular = pltpu.SemaphoreType.REGULAR
    return pl.pallas_call(
        functools.partial(kernel, groups, members),
        out_shape=(
            jax.ShapeDtypeStruct(fields.shape, jnp.float32),
            jax.ShapeDtypeStruct((2, depth * members, share, width), jnp.float32),
        ),
        in_specs=[
            pl.BlockSpec(memory_space=pltpu.HBM),
            pl.BlockSpec(memory_space=pltpu.HBM),
            pl.BlockSpec(memory_space=pltpu.HBM),
        ],
        out_specs=(pl.BlockSpec(memory_space=pltpu.VMEM), pl.BlockSpec(memory_space=pl.ANY)),
        scratch_shapes=[
            pltpu.VMEM((F, depth, rows + 16, width), jnp.float32),
            pltpu.VMEM((2, F, depth, rows, width), jnp.float32),
            pltpu.VMEM((F, depth, rows, width), jnp.float32),
            pltpu.VMEM((F, depth, ROWS, width), jnp.float32),
            pltpu.VMEM((F, F, 8, 128), jnp.float32),
            pltpu.VMEM((F, F, 8, 128), jnp.float32),
            pltpu.VMEM((members, 2, depth, share, width), jnp.float32),
            pltpu.VMEM((F, F), jnp.float32),
            pltpu.VMEM((F, F), jnp.float32),
            pltpu.VMEM((2, F, F, 128), jnp.float32),
            dma((6,)), dma((chunks,)), dma((chunks,)), dma((chunks,)), dma((chunks,)), dma((chunks,)), dma((chunks,)),
            dma, dma, dma, regular, regular, regular,
        ],
        compiler_params=pltpu.CompilerParams(
            collective_id=0, has_side_effects=True, vmem_limit_bytes=40 * 1024 * 1024
        ),
    )(*arrays)


def solution(mesh):
    groups, members = mesh.shape["grp"], mesh.shape["dev"]
    return jax.shard_map(
        functools.partial(per_device, groups, members),
        mesh=mesh,
        in_specs=(P(None, ("grp", "dev"), None, None), P(), P()),
        out_specs=(P(None, ("grp", "dev"), None, None), P(None, "grp", "dev", None)),
        check_vma=False,
    )
```

```python
import functools

import jax
import jax.numpy as jnp
from jax import lax
from jax.experimental import pallas as pl
from jax.experimental.pallas import tpu as pltpu
from jax.sharding import PartitionSpec as P

MESH = pl.DeviceIdType.MESH
F = 24
HALF = 12
ROWS = 8
LAG = 8
PIECES = 2
HOLD_P = 3
HOLD_R = 2
HOLD_D = 4
HOLD_V = 5
PARTS = 8
BLOCK = 12
COMPUTE = True
WEYL = True


def d12(m2, m1, p1, p2):
    return 8.0 * (p1 - m1) - (p2 - m2)


def kernel(groups, members, fields, mix_in, lap_in, rhs, weyl, own, halo, via, tsum, w1, w2, wl,
           mix, lapw, wrow, load_sem, send_p, recv_p, send_r, recv_r, send_d, recv_d, wsend, wrecv, wlocal,
           up, far, ready):
    depth = fields.shape[1]
    rows = fields.shape[2]
    width = fields.shape[3]
    tiles = rows // ROWS
    steps = 2 * tiles
    share = rows // members
    g = lax.axis_index("grp")
    d = lax.axis_index("dev")
    slabs = groups * members
    s = g * members + d
    odd = lax.rem(d, 2)
    partner = d + 1 - 2 * odd
    target = lax.rem(s + 2 - 4 * odd + slabs, slabs)
    target_id = {"grp": target // members, "dev": lax.rem(target, members)}
    end = members - 1
    godd = lax.rem(g, 2)

    def group(by):
        return {"grp": lax.rem(g + by + groups, groups)}

    hub = ((godd == 1) & (d == end - 1)) | ((godd == 0) & (d == 1))
    direct = ((godd == 1) & (d == end)) | ((godd == 0) & (d == 0))
    relays = jnp.logical_not(hub)
    hub_id = {"grp": lax.rem(g + 1 - 2 * godd + groups, groups), "dev": jnp.where(d == 0, end - 1, 1)}
    hub_target = {**group(2), "dev": jnp.where(d == 1, 0, end)}

    loads = []
    for half in range(2):
        part = pl.ds(half * HALF, HALF)
        loads.append(pltpu.make_async_copy(
            fields.at[part], own.at[part, :, pl.ds(8, rows), :], load_sem.at[half]))
    loads.append(pltpu.make_async_copy(
        fields.at[:, :, pl.ds(rows - 8, 8), :], own.at[:, :, pl.ds(0, 8), :], load_sem.at[2]))
    loads.append(pltpu.make_async_copy(
        fields.at[:, :, pl.ds(0, 8), :], own.at[:, :, pl.ds(rows + 8, 8), :], load_sem.at[3]))
    loads.append(pltpu.make_async_copy(mix_in, mix, load_sem.at[4]))
    loads.append(pltpu.make_async_copy(lap_in, lapw, load_sem.at[5]))
    for load in loads:
        load.start()

    barrier = pltpu.get_barrier_semaphore()

    def hello(to):
        pl.semaphore_signal(barrier, inc=1, device_id=to, device_id_type=MESH)

    def greet(to, _):
        hello({"dev": to})
        return 0

    @pl.when(odd == 1)
    def _():
        hello({"dev": d - 1})

    lax.fori_loop(d + 1, members, greet, 0)

    @pl.when((d == 0) & (godd == 1))
    def _():
        hello({**group(-1), "dev": end - 1})

    @pl.when((d == 1) & (godd == 1))
    def _():
        hello({**group(-1), "dev": end})

    @pl.when((d == 0) & (godd == 0))
    def _():
        hello({**group(1), "dev": end - 1})
        hello({**group(2), "dev": 1})

    @pl.when((d == 1) & (godd == 0))
    def _():
        hello({**group(1), "dev": end})

    @pl.when((d == end) & (godd == 1))
    def _():
        hello({**group(2), "dev": end - 1})

    extra = jnp.where(d == end, 1, jnp.where(d == end - 1, 1 + godd, jnp.where(d == 1, 1 - godd, 0)))
    pl.semaphore_wait(barrier, d + (1 - odd) + extra)

    size = HALF // PIECES
    last = PIECES + steps - 2

    def window(k, kind):
        if kind == 0:
            return pl.ds(k * size, size), 0
        if kind == 2:
            return pl.ds(HALF + (k - last) * size, size), rows - ROWS
        part = k - (PIECES - 1)
        return pl.ds((part // tiles) * HALF, HALF), pl.multiple_of(lax.rem(part, tiles) * ROWS, ROWS)

    def run(kind, first, stop, body):
        def once(k, _):
            body(k, kind)
            return 0
        lax.fori_loop(first, stop, once, 0)

    def each(body, low=0, high=steps):
        if low == 0:
            run(0, 0, PIECES, body)
        run(1, max(low, 1) + PIECES - 1, min(high, steps - 1) + PIECES - 1, body)
        if high == steps:
            run(2, last, last + PIECES, body)

    def at(part, body):
        @pl.when(part == 0)
        def _():
            run(0, 0, PIECES, body)

        @pl.when((part > 0) & (part < steps - 1))
        def _():
            body(part + PIECES - 1, 1)

        @pl.when(part == steps - 1)
        def _():
            run(2, last, last + PIECES, body)

    def own_chunk(k, kind):
        part, r0 = window(k, kind)
        return own.at[part, :, pl.ds(r0 + 8, ROWS), :]

    def halo_chunk(slot, k, kind):
        part, r0 = window(k, kind)
        return halo.at[slot, part, :, pl.ds(r0, ROWS), :]

    def via_chunk(k, kind):
        part, r0 = window(k, kind)
        return via.at[part, :, pl.ds(r0, ROWS), :]

    mine = 1 - odd

    def to_partner(k, kind):
        return pltpu.make_async_remote_copy(
            own_chunk(k, kind), halo_chunk(odd, k, kind), send_p.at[k], recv_p.at[k],
            device_id={"dev": partner}, device_id_type=MESH)

    def relay(k, kind):
        return pltpu.make_async_remote_copy(
            halo_chunk(mine, k, kind), halo_chunk(odd, k, kind), send_r.at[k], recv_r.at[k],
            device_id=target_id, device_id_type=MESH)

    def straight(k, kind):
        return pltpu.make_async_remote_copy(
            own_chunk(k, kind), via_chunk(k, kind), send_d.at[k], recv_d.at[k],
            device_id=hub_id, device_id_type=MESH)

    def hand_on(k, kind):
        return pltpu.make_async_remote_copy(
            via_chunk(k, kind), halo_chunk(mine, k, kind), send_r.at[k], recv_r.at[k],
            device_id=hub_target, device_id_type=MESH)

    def send(k, kind):
        to_partner(k, kind).start()

    def send_straight(k, kind):
        straight(k, kind).start()

    yields = (d == end) & (godd == 1)

    loads[0].wait()

    @pl.when(jnp.logical_not(yields))
    def _():
        each(send, 0, tiles)

    @pl.when((odd == 0) & (d >= 2))
    def _():
        pl.semaphore_signal(up, inc=1, device_id={"dev": d - 2}, device_id_type=MESH)

    @pl.when((d == end) & (godd == 0))
    def _():
        pl.semaphore_signal(up, inc=1, device_id={**group(1), "dev": 1}, device_id_type=MESH)

    @pl.when((d == end - 1) & (godd == 1))
    def _():
        pl.semaphore_signal(far, inc=1, device_id={**group(-1), "dev": 0}, device_id_type=MESH)

    loads[1].wait()

    @pl.when(jnp.logical_not(yields))
    def _():
        each(send, tiles, steps)

    @pl.when(yields)
    def _():
        each(send_straight)

    def reply(to, _):
        pl.semaphore_signal(ready, inc=1, device_id={"dev": to}, device_id_type=MESH)
        return 0

    lax.fori_loop(0, d, reply, 0)
    loads[2].wait()
    loads[3].wait()

    loads[4].wait()
    loads[5].wait()
    if COMPUTE:
        lap_all = lapw[...]
        for slot, table in enumerate((mix[...] - 7.5 * lap_all, lap_all * (1.0 / 12.0))):
            for h in range(F):
                wrow[slot, h] = jnp.broadcast_to(table[:, h:h + 1], (F, 128))

        def spread(h, _):
            for slot, into in enumerate((w1, w2)):
                for c in range(F):
                    into[h, c] = jnp.broadcast_to(wrow[slot, h, c:c + 1, :], (8, 128))
            return 0

        lax.fori_loop(0, F, spread, 0)

    lane = lax.broadcasted_iota(jnp.int32, (ROWS, width), 1).astype(jnp.float32)
    line = lax.broadcasted_iota(jnp.int32, (ROWS, width), 0).astype(jnp.float32)

    def near(h, r0, p, halos=True):
        def along(off):
            return own[h, p, pl.ds(r0 + 8 + off, ROWS), :]
        mid = pl.ds(pl.multiple_of(r0 + 8, 8), ROWS)
        here = own[h, p, mid, :]
        rows_at = pl.ds(pl.multiple_of(r0, 8), ROWS)
        xs = [pltpu.roll(here, 2, 1), pltpu.roll(here, 1, 1),
              pltpu.roll(here, width - 1, 1), pltpu.roll(here, width - 2, 1)]
        ys = [along(-2), along(-1), along(1), along(2)]
        other = own[h, 1 - p, mid, :]
        if not halos:
            return here, xs, ys, other
        if p == 0:
            zs = [halo[0, h, 0, rows_at, :], halo[0, h, 1, rows_at, :],
                  other, halo[1, h, 0, rows_at, :]]
        else:
            zs = [halo[0, h, 1, rows_at, :], other,
                  halo[1, h, 0, rows_at, :], halo[1, h, 1, rows_at, :]]
        return here, xs, ys, zs

    def lap_sum(xs, ys, zs):
        one = (xs[1] + xs[2]) + (ys[1] + ys[2]) + (zs[1] + zs[2])
        two = (xs[0] + xs[3]) + (ys[0] + ys[3]) + (zs[0] + zs[3])
        return 16.0 * one - two

    def weyl_tile(tile):
        r0 = tile * ROWS
        xpos = lane + (0.5 - 0.5 * width)
        ypos = line + (r0.astype(jnp.float32) + (0.5 - 0.5 * rows))
        sq = xpos * xpos + ypos * ypos
        inv_s = lax.rsqrt(sq)
        cyl = sq * inv_s
        cosp = xpos * inv_s
        sinp = ypos * inv_s
        for p in range(depth):
            zpos = (s * depth + p).astype(jnp.float32) + (0.5 - 0.5 * slabs * depth)
            inv_r = lax.rsqrt(sq + zpos * zpos)
            zr = zpos * inv_r
            theta = (zr * cosp, zr * sinp, -(cyl * inv_r))
            phi = (-sinp, cosp)
            curv = []
            grad = []
            for h in range(6, 12):
                here, xs, ys, zs = near(h, r0, p)
                curv.append(here)
                grad.append((d12(*xs), d12(*ys), d12(*zs)))
            trace = curv[0] + curv[3] + curv[5]
            table = ((0, 1, 2), (1, 3, 4), (2, 4, 5))
            pairs = ((0, 0), (0, 1), (0, 2), (1, 1), (1, 2), (2, 2))

            def curl(i, j):
                n1, n2 = (i + 1) % 3, (i + 2) % 3
                return grad[table[n2][j]][n1] - grad[table[n1][j]][n2]

            real = None
            imag = None
            for comp, (i, j) in enumerate(pairs):
                here, xs, ys, zs = near(comp, r0, p)
                lap = lap_sum(xs, ys, zs) - 90.0 * here
                elec = lap * (-0.5 / 12.0) - trace * curv[comp]
                for m in range(3):
                    elec = elec + curv[table[i][m]] * curv[table[m][j]]
                if i == j:
                    mag = curl(i, i) * (1.0 / 12.0)
                else:
                    mag = (curl(i, j) + curl(j, i)) * (0.5 / 12.0)
                fi = phi[i] if i < 2 else None
                fj = phi[j] if j < 2 else None
                tt = theta[i] * theta[j]
                both = tt if fi is None or fj is None else tt - fi * fj
                mixed = None
                for u, v in ((theta[i], fj), (theta[j], fi)):
                    if v is not None:
                        mixed = u * v if mixed is None else mixed + u * v
                if i == j:
                    both = 0.5 * both
                    mixed = None if mixed is None else 0.5 * mixed
                one = elec * both
                two = mag * both
                if mixed is not None:
                    one = one - mag * mixed
                    two = two + elec * mixed
                real = one if real is None else real + one
                imag = two if imag is None else imag + two
            imag = -imag
            per = ROWS // share
            for k in range(per):
                wl[tile * per + k, 0, p] = real[k * share:(k + 1) * share]
                wl[tile * per + k, 1, p] = imag[k * share:(k + 1) * share]

    def weyl_send(tile):
        per = ROWS // share
        for k in range(per):
            to = tile * per + k

            @pl.when(to == d)
            def _():
                pltpu.make_async_copy(
                    wl.at[to], weyl.at[:, pl.ds(d * depth, depth)], wlocal).start()

            @pl.when(to != d)
            def _():
                pltpu.make_async_remote_copy(
                    wl.at[to], weyl.at[:, pl.ds(d * depth, depth)], wsend, wrecv,
                    device_id={"dev": to}, device_id_type=MESH).start()

    def mixed(tile, h0, h1, with_own):
        mid = pl.ds(pl.multiple_of(tile * ROWS + 8, 8), ROWS)
        out = pl.ds(pl.multiple_of(tile * ROWS, 8), ROWS)
        for c0 in range(0, F, BLOCK):
            def mixing(h4, acc):
                for k in range(4):
                    h = h4 * 4 + k
                    if with_own:
                        acc = acc + w1[h, pl.ds(c0, BLOCK)][:, None] * own[h, :, mid, :][None]
                    acc = acc + w2[h, pl.ds(c0, BLOCK)][:, None] * tsum[h][None]
                return acc
            start = rhs[pl.ds(c0, BLOCK), :, out, :]
            rhs[pl.ds(c0, BLOCK), :, out, :] = lax.fori_loop(h0 // 4, h1 // 4, mixing, start)

    def rhs_early(tile):
        r0 = tile * ROWS
        mid = pl.ds(pl.multiple_of(r0 + 8, 8), ROWS)
        out = pl.ds(pl.multiple_of(r0, 8), ROWS)

        def stencil(halos, h4, _):
            for p in range(depth):
                bz = own[12, p, mid, :] * (1.0 / 12.0)
                by = own[13, p, mid, :] * (1.0 / 12.0)
                bx = own[14, p, mid, :] * (1.0 / 12.0)
                for k in range(4):
                    h = h4 * 4 + k
                    here, xs, ys, zs = near(h, r0, p, halos)
                    if halos:
                        tsum[h, p] = lap_sum(xs, ys, zs)
                        dz = d12(*zs)
                    else:
                        one = (xs[1] + xs[2]) + (ys[1] + ys[2]) + zs
                        two = (xs[0] + xs[3]) + (ys[0] + ys[3])
                        tsum[h, p] = 16.0 * one - two
                        dz = (8.0 if p == 0 else -8.0) * zs
                    rhs[h, p, out, :] = bx * d12(*xs) + by * d12(*ys) + bz * dz
            return 0

        lax.fori_loop(0, HALF // 4, functools.partial(stencil, True), 0)
        lax.fori_loop(HALF // 4, F // 4, functools.partial(stencil, False), 0)
        mixed(tile, 0, F, True)

    def rhs_late(tile):
        r0 = tile * ROWS
        mid = pl.ds(pl.multiple_of(r0 + 8, 8), ROWS)
        out = pl.ds(pl.multiple_of(r0, 8), ROWS)

        def planes(h4, _):
            for p in range(depth):
                bz = own[12, p, mid, :] * (1.0 / 12.0)
                for k in range(4):
                    h = h4 * 4 + k
                    below = halo[0, h, 1, out, :]
                    above = halo[1, h, 0, out, :]
                    if p == 0:
                        far = halo[0, h, 0, out, :]
                        tsum[h, p] = 16.0 * below - (far + above)
                        dz = (far - above) - 8.0 * below
                    else:
                        far = halo[1, h, 1, out, :]
                        tsum[h, p] = 16.0 * above - (below + far)
                        dz = 8.0 * above + (below - far)
                    rhs[h, p, out, :] = rhs[h, p, out, :] + bz * dz
            return 0

        lax.fori_loop(HALF // 4, F // 4, planes, 0)
        mixed(tile, HALF, F, False)

    asks = ((odd == 0) & (d < end - 1)) | ((d == 1) & (godd == 1))
    held = (d == 1) & (godd == 1)
    hold_hub = jnp.where(d == 1, HOLD_V, 1)

    def ask():
        @pl.when(asks)
        def _():
            pl.semaphore_wait(up, 1)

    def arrived(k, kind):
        to_partner(k, kind).wait_recv()

        @pl.when(relays & jnp.logical_not(held))
        def _():
            relay(k, kind).start()

    def late_relay(k, kind):
        relay(k, kind).start()

    def pass_on(k, kind):
        straight(k, kind).wait_recv()
        hand_on(k, kind).start()

    def done(k, kind):
        relay(k, kind).wait_recv()
        to_partner(k, kind).wait_send()
        relay(k, kind).wait_send()

        @pl.when(direct)
        def _():
            straight(k, kind).wait_send()

    def passed(part):
        return jnp.minimum(jnp.minimum(jnp.maximum(2 * (part - hold_hub), 0), part), steps)

    def step(part, _):
        @pl.when((part == 0) & jnp.logical_not(held))
        def _():
            ask()

        at(part, arrived)

        @pl.when(held)
        def _():
            @pl.when(part == HOLD_R)
            def _():
                ask()
            at(part - HOLD_R, late_relay)

        @pl.when(yields & (part == HOLD_P))
        def _():
            each(send)

        @pl.when(direct & (d == 0) & (part == HOLD_D))
        def _():
            pl.semaphore_wait(far, 1)
            each(send_straight)

        @pl.when(hub)
        def _():
            def catch_up(v, _):
                at(v, pass_on)
                return 0
            lax.fori_loop(passed(part), passed(part + 1), catch_up, 0)

        j = part - LAG
        at(j, done)

        @pl.when((j == 1) & (d < end))
        def _():
            pl.semaphore_wait(ready, end - d)

        if WEYL:
            @pl.when((j >= 1) & (j <= tiles))
            def _():
                weyl_send(j - 1)

        if COMPUTE:
            @pl.when((j >= 0) & (j < tiles))
            def _():
                weyl_tile(j)
                rhs_early(j)

            @pl.when(j >= tiles)
            def _():
                rhs_late(j - tiles)
        return 0

    lax.fori_loop(0, steps + LAG, step, 0)

    if WEYL:
        sent = wl.at[pl.ds(0, members - 1)]
        pltpu.make_async_copy(sent, sent, wsend).wait()
        came = weyl.at[:, pl.ds(0, depth * (members - 1))]
        pltpu.make_async_copy(came, came, wrecv).wait()
        pltpu.make_async_copy(wl.at[0], weyl.at[:, pl.ds(0, depth)], wlocal).wait()


def put_out(rhs_in, weyl_in, rhs, weyl, sem):
    each = F // PARTS
    copies = [pltpu.make_async_copy(weyl_in, weyl, sem.at[PARTS])]
    for k in range(PARTS):
        part = pl.ds(k * each, each)
        copies.append(pltpu.make_async_copy(rhs_in.at[part], rhs.at[part], sem.at[k]))
    for copy in copies:
        copy.start()
    for copy in copies:
        copy.wait()


def per_device(groups, members, fields, mix_matrix, laplace_matrix):
    depth, rows, width = fields.shape[1:]
    share = rows // members
    chunks = 2 * (rows // ROWS) - 2 + 2 * PIECES
    arrays = [pltpu.with_memory_space_constraint(a, pltpu.HBM)
              for a in (fields, mix_matrix, laplace_matrix)]
    dma = pltpu.SemaphoreType.DMA
    regular = pltpu.SemaphoreType.REGULAR
    shapes = (fields.shape, (2, depth * members, share, width))
    results = pl.pallas_call(
        functools.partial(kernel, groups, members),
        out_shape=tuple(pltpu.VMEM(shape, jnp.float32) for shape in shapes),
        in_specs=[
            pl.BlockSpec(memory_space=pltpu.HBM),
            pl.BlockSpec(memory_space=pltpu.HBM),
            pl.BlockSpec(memory_space=pltpu.HBM),
        ],
        out_specs=(pl.BlockSpec(memory_space=pltpu.VMEM), pl.BlockSpec(memory_space=pl.ANY)),
        scratch_shapes=[
            pltpu.VMEM((F, depth, rows + 16, width), jnp.float32),
            pltpu.VMEM((2, F, depth, rows, width), jnp.float32),
            pltpu.VMEM((F, depth, rows, width), jnp.float32),
            pltpu.VMEM((F, depth, ROWS, width), jnp.float32),
            pltpu.VMEM((F, F, 8, 128), jnp.float32),
            pltpu.VMEM((F, F, 8, 128), jnp.float32),
            pltpu.VMEM((members, 2, depth, share, width), jnp.float32),
            pltpu.VMEM((F, F), jnp.float32),
            pltpu.VMEM((F, F), jnp.float32),
            pltpu.VMEM((2, F, F, 128), jnp.float32),
            dma((6,)), dma((chunks,)), dma((chunks,)), dma((chunks,)), dma((chunks,)), dma((chunks,)), dma((chunks,)),
            dma, dma, dma, regular, regular, regular,
        ],
        compiler_params=pltpu.CompilerParams(
            collective_id=0, has_side_effects=True, vmem_limit_bytes=40 * 1024 * 1024
        ),
    )(*arrays)
    return pl.pallas_call(
        put_out,
        out_shape=tuple(pltpu.HBM(shape, jnp.float32) for shape in shapes),
        in_specs=[pl.BlockSpec(memory_space=pltpu.VMEM)] * 2,
        out_specs=(pl.BlockSpec(memory_space=pltpu.HBM),) * 2,
        scratch_shapes=[pltpu.SemaphoreType.DMA((PARTS + 1,))],
        compiler_params=pltpu.CompilerParams(vmem_limit_bytes=1024 * 1024),
    )(*results)


def solution(mesh):
    groups, members = mesh.shape["grp"], mesh.shape["dev"]
    return jax.shard_map(
        functools.partial(per_device, groups, members),
        mesh=mesh,
        in_specs=(P(None, ("grp", "dev"), None, None), P(), P()),
        out_specs=(P(None, ("grp", "dev"), None, None), P(None, "grp", "dev", None)),
        check_vma=False,
    )
```

```python
import functools

import jax
import jax.numpy as jnp
from jax import lax
from jax.experimental import pallas as pl
from jax.experimental.pallas import tpu as pltpu
from jax.sharding import PartitionSpec as P

MESH = pl.DeviceIdType.MESH
F = 24
HALF = 12
ROWS = 8
LAG = 8
PIECES = 2
HOLD_P = 1
HOLD_R = 2
HOLD_D = 4
HOLD_V = 5
PARTS = 8
AHEAD = 20
TURN_END = 24
EVERY = 8
HOLD_F = 3
BLOCK = 12
COMPUTE = True
WEYL = True


def d12(m2, m1, p1, p2):
    return 8.0 * (p1 - m1) - (p2 - m2)


def kernel(groups, members, fields, mix_in, lap_in, rhs, weyl, own, halo, via, tsum, w1, w2, wl,
           mix, lapw, wrow, load_sem, send_p, recv_p, send_r, recv_r, send_d, recv_d, wsend, wrecv, wlocal,
           up, far, ready, send_f, over):
    depth = fields.shape[1]
    rows = fields.shape[2]
    width = fields.shape[3]
    tiles = rows // ROWS
    steps = 2 * tiles
    share = rows // members
    g = lax.axis_index("grp")
    d = lax.axis_index("dev")
    slabs = groups * members
    s = g * members + d
    odd = lax.rem(d, 2)
    partner = d + 1 - 2 * odd
    target = lax.rem(s + 2 - 4 * odd + slabs, slabs)
    target_id = {"grp": target // members, "dev": lax.rem(target, members)}
    end = members - 1
    godd = lax.rem(g, 2)

    def group(by):
        return {"grp": lax.rem(g + by + groups, groups)}

    hub = ((godd == 1) & (d == end - 1)) | ((godd == 0) & (d == 1))
    direct = ((godd == 1) & (d == end)) | ((godd == 0) & (d == 0))
    relays = jnp.logical_not(hub)
    hub_id = {"grp": lax.rem(g + 1 - 2 * godd + groups, groups), "dev": jnp.where(d == 0, end - 1, 1)}
    hub_target = {**group(2), "dev": jnp.where(d == 1, 0, end)}

    loads = []
    for half in range(2):
        part = pl.ds(half * HALF, HALF)
        loads.append(pltpu.make_async_copy(
            fields.at[part], own.at[part, :, pl.ds(8, rows), :], load_sem.at[half]))
    loads.append(pltpu.make_async_copy(
        fields.at[:, :, pl.ds(rows - 8, 8), :], own.at[:, :, pl.ds(0, 8), :], load_sem.at[2]))
    loads.append(pltpu.make_async_copy(
        fields.at[:, :, pl.ds(0, 8), :], own.at[:, :, pl.ds(rows + 8, 8), :], load_sem.at[3]))
    loads.append(pltpu.make_async_copy(mix_in, mix, load_sem.at[4]))
    loads.append(pltpu.make_async_copy(lap_in, lapw, load_sem.at[5]))
    for load in loads:
        load.start()

    barrier = pltpu.get_barrier_semaphore()

    def hello(to):
        pl.semaphore_signal(barrier, inc=1, device_id=to, device_id_type=MESH)

    def greet(to, _):
        hello({"dev": to})
        return 0

    @pl.when(odd == 1)
    def _():
        hello({"dev": d - 1})

    lax.fori_loop(d + 1, members, greet, 0)

    @pl.when((d == 0) & (godd == 1))
    def _():
        hello({**group(-1), "dev": end - 1})

    @pl.when((d == 1) & (godd == 1))
    def _():
        hello({**group(-1), "dev": end})

    @pl.when((d == 0) & (godd == 0))
    def _():
        hello({**group(1), "dev": end - 1})
        hello({**group(2), "dev": 1})

    @pl.when((d == 1) & (godd == 0))
    def _():
        hello({**group(1), "dev": end})

    @pl.when((d == end) & (godd == 1))
    def _():
        hello({**group(2), "dev": end - 1})

    wide = ((odd == 0) & (d <= end - 3)) | ((odd == 1) & (d >= 3))

    @pl.when((odd == 0) & (d <= end - 3))
    def _():
        hello({**group(2), "dev": d + 3})

    @pl.when((odd == 0) & (d >= 2))
    def _():
        hello({**group(2), "dev": d + 1})

    @pl.when((odd == 1) & (d < end))
    def _():
        hello({**group(2), "dev": d - 1})

    wider = jnp.where(wide, 1 + odd, 0)
    extra = wider + jnp.where(d == end, 1, jnp.where(d == end - 1, 1 + godd, jnp.where(d == 1, 1 - godd, 0)))
    pl.semaphore_wait(barrier, d + (1 - odd) + extra)

    size = HALF // PIECES
    last = PIECES + steps - 2

    def window(k, kind):
        if kind == 0:
            return pl.ds(k * size, size), 0
        if kind == 2:
            return pl.ds(HALF + (k - last) * size, size), rows - ROWS
        part = k - (PIECES - 1)
        return pl.ds((part // tiles) * HALF, HALF), pl.multiple_of(lax.rem(part, tiles) * ROWS, ROWS)

    def run(kind, first, stop, body):
        def once(k, _):
            body(k, kind)
            return 0
        lax.fori_loop(first, stop, once, 0)

    def each(body, low=0, high=steps):
        if low == 0:
            run(0, 0, PIECES, body)
        run(1, max(low, 1) + PIECES - 1, min(high, steps - 1) + PIECES - 1, body)
        if high == steps:
            run(2, last, last + PIECES, body)

    def at(part, body):
        @pl.when(part == 0)
        def _():
            run(0, 0, PIECES, body)

        @pl.when((part > 0) & (part < steps - 1))
        def _():
            body(part + PIECES - 1, 1)

        @pl.when(part == steps - 1)
        def _():
            run(2, last, last + PIECES, body)

    def own_chunk(k, kind):
        part, r0 = window(k, kind)
        return own.at[part, :, pl.ds(r0 + 8, ROWS), :]

    def halo_chunk(slot, k, kind):
        part, r0 = window(k, kind)
        return halo.at[slot, part, :, pl.ds(r0, ROWS), :]

    def via_chunk(k, kind):
        part, r0 = window(k, kind)
        return via.at[part, :, pl.ds(r0, ROWS), :]

    mine = 1 - odd

    def to_partner(k, kind):
        return pltpu.make_async_remote_copy(
            own_chunk(k, kind), halo_chunk(odd, k, kind), send_p.at[k], recv_p.at[k],
            device_id={"dev": partner}, device_id_type=MESH)

    def relay(k, kind):
        return pltpu.make_async_remote_copy(
            halo_chunk(mine, k, kind), halo_chunk(odd, k, kind), send_r.at[k], recv_r.at[k],
            device_id=target_id, device_id_type=MESH)

    def straight(k, kind):
        return pltpu.make_async_remote_copy(
            own_chunk(k, kind), via_chunk(k, kind), send_d.at[k], recv_d.at[k],
            device_id=hub_id, device_id_type=MESH)

    def hand_on(k, kind):
        return pltpu.make_async_remote_copy(
            via_chunk(k, kind), halo_chunk(mine, k, kind), send_r.at[k], recv_r.at[k],
            device_id=hub_target, device_id_type=MESH)

    def detour(k, kind):
        return pltpu.make_async_remote_copy(
            halo_chunk(mine, k, kind), via_chunk(k, kind), send_r.at[k], recv_d.at[k],
            device_id={**group(2), "dev": d + 3 - 6 * odd}, device_id_type=MESH)

    def hand_back(k, kind):
        return pltpu.make_async_remote_copy(
            via_chunk(k, kind), halo_chunk(mine, k, kind), send_f.at[k], recv_r.at[k],
            device_id={**group(2), "dev": partner}, device_id_type=MESH)

    def turn(part):
        return wide & (part > 0) & (part < TURN_END) & (lax.rem(part, EVERY) == EVERY - 1)

    def send(k, kind):
        to_partner(k, kind).start()

    def send_straight(k, kind):
        straight(k, kind).start()

    yields = (d == end) & (godd == 1)

    loads[0].wait()

    @pl.when(jnp.logical_not(yields))
    def _():
        each(send, 0, min(AHEAD, tiles))

    @pl.when((odd == 0) & (d >= 2))
    def _():
        pl.semaphore_signal(up, inc=1, device_id={"dev": d - 2}, device_id_type=MESH)

    @pl.when((odd == 1) & (d >= 3))
    def _():
        pl.semaphore_signal(over, inc=1, device_id={**group(2), "dev": d - 3}, device_id_type=MESH)

    @pl.when((d == end) & (godd == 0))
    def _():
        pl.semaphore_signal(up, inc=1, device_id={**group(1), "dev": 1}, device_id_type=MESH)

    @pl.when((d == end - 1) & (godd == 1))
    def _():
        pl.semaphore_signal(far, inc=1, device_id={**group(-1), "dev": 0}, device_id_type=MESH)

    loads[1].wait()

    if AHEAD > tiles:
        @pl.when(jnp.logical_not(yields))
        def _():
            each(send, tiles, AHEAD)

    @pl.when(yields)
    def _():
        each(send_straight)

    def reply(to, _):
        pl.semaphore_signal(ready, inc=1, device_id={"dev": to}, device_id_type=MESH)
        return 0

    lax.fori_loop(0, d, reply, 0)
    loads[2].wait()
    loads[3].wait()

    loads[4].wait()
    loads[5].wait()
    if COMPUTE:
        lap_all = lapw[...]
        for slot, table in enumerate((mix[...] - 7.5 * lap_all, lap_all * (1.0 / 12.0))):
            for h in range(F):
                wrow[slot, h] = jnp.broadcast_to(table[:, h:h + 1], (F, 128))

        def spread(h, _):
            for slot, into in enumerate((w1, w2)):
                for c in range(F):
                    into[h, c] = jnp.broadcast_to(wrow[slot, h, c:c + 1, :], (8, 128))
            return 0

        lax.fori_loop(0, F, spread, 0)

    lane = lax.broadcasted_iota(jnp.int32, (ROWS, width), 1).astype(jnp.float32)
    line = lax.broadcasted_iota(jnp.int32, (ROWS, width), 0).astype(jnp.float32)

    def near(h, r0, p, halos=True):
        def along(off):
            return own[h, p, pl.ds(r0 + 8 + off, ROWS), :]
        mid = pl.ds(pl.multiple_of(r0 + 8, 8), ROWS)
        here = own[h, p, mid, :]
        rows_at = pl.ds(pl.multiple_of(r0, 8), ROWS)
        xs = [pltpu.roll(here, 2, 1), pltpu.roll(here, 1, 1),
              pltpu.roll(here, width - 1, 1), pltpu.roll(here, width - 2, 1)]
        ys = [along(-2), along(-1), along(1), along(2)]
        other = own[h, 1 - p, mid, :]
        if not halos:
            return here, xs, ys, other
        if p == 0:
            zs = [halo[0, h, 0, rows_at, :], halo[0, h, 1, rows_at, :],
                  other, halo[1, h, 0, rows_at, :]]
        else:
            zs = [halo[0, h, 1, rows_at, :], other,
                  halo[1, h, 0, rows_at, :], halo[1, h, 1, rows_at, :]]
        return here, xs, ys, zs

    def lap_sum(xs, ys, zs):
        one = (xs[1] + xs[2]) + (ys[1] + ys[2]) + (zs[1] + zs[2])
        two = (xs[0] + xs[3]) + (ys[0] + ys[3]) + (zs[0] + zs[3])
        return 16.0 * one - two

    def weyl_tile(tile):
        r0 = tile * ROWS
        xpos = lane + (0.5 - 0.5 * width)
        ypos = line + (r0.astype(jnp.float32) + (0.5 - 0.5 * rows))
        sq = xpos * xpos + ypos * ypos
        inv_s = lax.rsqrt(sq)
        cyl = sq * inv_s
        cosp = xpos * inv_s
        sinp = ypos * inv_s
        for p in range(depth):
            zpos = (s * depth + p).astype(jnp.float32) + (0.5 - 0.5 * slabs * depth)
            inv_r = lax.rsqrt(sq + zpos * zpos)
            zr = zpos * inv_r
            theta = (zr * cosp, zr * sinp, -(cyl * inv_r))
            phi = (-sinp, cosp)
            curv = []
            grad = []
            for h in range(6, 12):
                here, xs, ys, zs = near(h, r0, p)
                curv.append(here)
                grad.append((d12(*xs), d12(*ys), d12(*zs)))
            trace = curv[0] + curv[3] + curv[5]
            table = ((0, 1, 2), (1, 3, 4), (2, 4, 5))
            pairs = ((0, 0), (0, 1), (0, 2), (1, 1), (1, 2), (2, 2))

            def curl(i, j):
                n1, n2 = (i + 1) % 3, (i + 2) % 3
                return grad[table[n2][j]][n1] - grad[table[n1][j]][n2]

            real = None
            imag = None
            for comp, (i, j) in enumerate(pairs):
                here, xs, ys, zs = near(comp, r0, p)
                lap = lap_sum(xs, ys, zs) - 90.0 * here
                elec = lap * (-0.5 / 12.0) - trace * curv[comp]
                for m in range(3):
                    elec = elec + curv[table[i][m]] * curv[table[m][j]]
                if i == j:
                    mag = curl(i, i) * (1.0 / 12.0)
                else:
                    mag = (curl(i, j) + curl(j, i)) * (0.5 / 12.0)
                fi = phi[i] if i < 2 else None
                fj = phi[j] if j < 2 else None
                tt = theta[i] * theta[j]
                both = tt if fi is None or fj is None else tt - fi * fj
                mixed = None
                for u, v in ((theta[i], fj), (theta[j], fi)):
                    if v is not None:
                        mixed = u * v if mixed is None else mixed + u * v
                if i == j:
                    both = 0.5 * both
                    mixed = None if mixed is None else 0.5 * mixed
                one = elec * both
                two = mag * both
                if mixed is not None:
                    one = one - mag * mixed
                    two = two + elec * mixed
                real = one if real is None else real + one
                imag = two if imag is None else imag + two
            imag = -imag
            per = ROWS // share
            for k in range(per):
                wl[tile * per + k, 0, p] = real[k * share:(k + 1) * share]
                wl[tile * per + k, 1, p] = imag[k * share:(k + 1) * share]

    def weyl_send(tile):
        per = ROWS // share
        for k in range(per):
            to = tile * per + k

            @pl.when(to == d)
            def _():
                pltpu.make_async_copy(
                    wl.at[to], weyl.at[:, pl.ds(d * depth, depth)], wlocal).start()

            @pl.when(to != d)
            def _():
                pltpu.make_async_remote_copy(
                    wl.at[to], weyl.at[:, pl.ds(d * depth, depth)], wsend, wrecv,
                    device_id={"dev": to}, device_id_type=MESH).start()

    def mixed(tile, h0, h1, with_own):
        mid = pl.ds(pl.multiple_of(tile * ROWS + 8, 8), ROWS)
        out = pl.ds(pl.multiple_of(tile * ROWS, 8), ROWS)
        for c0 in range(0, F, BLOCK):
            def mixing(h4, acc):
                for k in range(4):
                    h = h4 * 4 + k
                    if with_own:
                        acc = acc + w1[h, pl.ds(c0, BLOCK)][:, None] * own[h, :, mid, :][None]
                    acc = acc + w2[h, pl.ds(c0, BLOCK)][:, None] * tsum[h][None]
                return acc
            start = rhs[pl.ds(c0, BLOCK), :, out, :]
            rhs[pl.ds(c0, BLOCK), :, out, :] = lax.fori_loop(h0 // 4, h1 // 4, mixing, start)

    def rhs_early(tile):
        r0 = tile * ROWS
        mid = pl.ds(pl.multiple_of(r0 + 8, 8), ROWS)
        out = pl.ds(pl.multiple_of(r0, 8), ROWS)

        def stencil(halos, h4, _):
            for p in range(depth):
                bz = own[12, p, mid, :] * (1.0 / 12.0)
                by = own[13, p, mid, :] * (1.0 / 12.0)
                bx = own[14, p, mid, :] * (1.0 / 12.0)
                for k in range(4):
                    h = h4 * 4 + k
                    here, xs, ys, zs = near(h, r0, p, halos)
                    if halos:
                        tsum[h, p] = lap_sum(xs, ys, zs)
                        dz = d12(*zs)
                    else:
                        one = (xs[1] + xs[2]) + (ys[1] + ys[2]) + zs
                        two = (xs[0] + xs[3]) + (ys[0] + ys[3])
                        tsum[h, p] = 16.0 * one - two
                        dz = (8.0 if p == 0 else -8.0) * zs
                    rhs[h, p, out, :] = bx * d12(*xs) + by * d12(*ys) + bz * dz
            return 0

        lax.fori_loop(0, HALF // 4, functools.partial(stencil, True), 0)
        lax.fori_loop(HALF // 4, F // 4, functools.partial(stencil, False), 0)
        mixed(tile, 0, F, True)

    def rhs_late(tile):
        r0 = tile * ROWS
        mid = pl.ds(pl.multiple_of(r0 + 8, 8), ROWS)
        out = pl.ds(pl.multiple_of(r0, 8), ROWS)

        def planes(h4, _):
            for p in range(depth):
                bz = own[12, p, mid, :] * (1.0 / 12.0)
                for k in range(4):
                    h = h4 * 4 + k
                    below = halo[0, h, 1, out, :]
                    above = halo[1, h, 0, out, :]
                    if p == 0:
                        far = halo[0, h, 0, out, :]
                        tsum[h, p] = 16.0 * below - (far + above)
                        dz = (far - above) - 8.0 * below
                    else:
                        far = halo[1, h, 1, out, :]
                        tsum[h, p] = 16.0 * above - (below + far)
                        dz = 8.0 * above + (below - far)
                    rhs[h, p, out, :] = rhs[h, p, out, :] + bz * dz
            return 0

        lax.fori_loop(HALF // 4, F // 4, planes, 0)
        mixed(tile, HALF, F, False)

    asks = ((odd == 0) & (d < end - 1)) | ((d == 1) & (godd == 1))
    held = (d == 1) & (godd == 1)
    hold_hub = jnp.where(d == 1, HOLD_V, 1)

    def ask():
        @pl.when(asks)
        def _():
            pl.semaphore_wait(up, 1)

    def arrived(k, kind):
        to_partner(k, kind).wait_recv()
        if kind == 1:
            astray = turn(k - (PIECES - 1))

            @pl.when(astray)
            def _():
                detour(k, kind).start()

            @pl.when(relays & jnp.logical_not(held | astray))
            def _():
                relay(k, kind).start()
        else:
            @pl.when(relays & jnp.logical_not(held))
            def _():
                relay(k, kind).start()

    def late_relay(k, kind):
        relay(k, kind).start()

    def pass_on(k, kind):
        straight(k, kind).wait_recv()
        hand_on(k, kind).start()

    def done(k, kind):
        relay(k, kind).wait_recv()
        to_partner(k, kind).wait_send()
        relay(k, kind).wait_send()
        if kind == 1:
            @pl.when(turn(k - (PIECES - 1)))
            def _():
                hand_back(k, kind).wait_send()

        @pl.when(direct)
        def _():
            straight(k, kind).wait_send()

    def passed(part):
        return jnp.minimum(jnp.minimum(jnp.maximum(2 * (part - hold_hub), 0), part), steps)

    def step(part, _):
        @pl.when((part == 0) & jnp.logical_not(held))
        def _():
            ask()

        @pl.when((part == EVERY - 1) & wide & (odd == 0))
        def _():
            pl.semaphore_wait(over, 1)

        at(part, arrived)

        @pl.when(turn(part - HOLD_F))
        def _():
            k = part - HOLD_F + PIECES - 1
            straight(k, 1).wait_recv()
            hand_back(k, 1).start()

        @pl.when(held)
        def _():
            @pl.when(part == HOLD_R)
            def _():
                ask()
            at(part - HOLD_R, late_relay)

        @pl.when(yields & (part == HOLD_P))
        def _():
            each(send, 0, AHEAD + HOLD_P)

        @pl.when(jnp.logical_not(yields & (part < HOLD_P)))
        def _():
            at(part + AHEAD, send)

        @pl.when(direct & (d == 0) & (part == HOLD_D))
        def _():
            pl.semaphore_wait(far, 1)
            each(send_straight)

        @pl.when(hub)
        def _():
            def catch_up(v, _):
                at(v, pass_on)
                return 0
            lax.fori_loop(passed(part), passed(part + 1), catch_up, 0)

        j = part - LAG
        at(j, done)

        @pl.when((j == 1) & (d < end))
        def _():
            pl.semaphore_wait(ready, end - d)

        if WEYL:
            @pl.when((j >= 1) & (j <= tiles))
            def _():
                weyl_send(j - 1)

        if COMPUTE:
            @pl.when((j >= 0) & (j < tiles))
            def _():
                weyl_tile(j)
                rhs_early(j)

            @pl.when(j >= tiles)
            def _():
                rhs_late(j - tiles)
        return 0

    lax.fori_loop(0, steps + LAG, step, 0)

    if WEYL:
        sent = wl.at[pl.ds(0, members - 1)]
        pltpu.make_async_copy(sent, sent, wsend).wait()
        came = weyl.at[:, pl.ds(0, depth * (members - 1))]
        pltpu.make_async_copy(came, came, wrecv).wait()
        pltpu.make_async_copy(wl.at[0], weyl.at[:, pl.ds(0, depth)], wlocal).wait()


def put_out(rhs_in, weyl_in, rhs, weyl, sem):
    each = F // PARTS
    copies = [pltpu.make_async_copy(weyl_in, weyl, sem.at[PARTS])]
    for k in range(PARTS):
        part = pl.ds(k * each, each)
        copies.append(pltpu.make_async_copy(rhs_in.at[part], rhs.at[part], sem.at[k]))
    for copy in copies:
        copy.start()
    for copy in copies:
        copy.wait()


def per_device(groups, members, fields, mix_matrix, laplace_matrix):
    depth, rows, width = fields.shape[1:]
    share = rows // members
    chunks = 2 * (rows // ROWS) - 2 + 2 * PIECES
    arrays = [pltpu.with_memory_space_constraint(a, pltpu.HBM)
              for a in (fields, mix_matrix, laplace_matrix)]
    dma = pltpu.SemaphoreType.DMA
    regular = pltpu.SemaphoreType.REGULAR
    shapes = (fields.shape, (2, depth * members, share, width))
    results = pl.pallas_call(
        functools.partial(kernel, groups, members),
        out_shape=tuple(pltpu.VMEM(shape, jnp.float32) for shape in shapes),
        in_specs=[
            pl.BlockSpec(memory_space=pltpu.HBM),
            pl.BlockSpec(memory_space=pltpu.HBM),
            pl.BlockSpec(memory_space=pltpu.HBM),
        ],
        out_specs=(pl.BlockSpec(memory_space=pltpu.VMEM), pl.BlockSpec(memory_space=pl.ANY)),
        scratch_shapes=[
            pltpu.VMEM((F, depth, rows + 16, width), jnp.float32),
            pltpu.VMEM((2, F, depth, rows, width), jnp.float32),
            pltpu.VMEM((F, depth, rows, width), jnp.float32),
            pltpu.VMEM((F, depth, ROWS, width), jnp.float32),
            pltpu.VMEM((F, F, 8, 128), jnp.float32),
            pltpu.VMEM((F, F, 8, 128), jnp.float32),
            pltpu.VMEM((members, 2, depth, share, width), jnp.float32),
            pltpu.VMEM((F, F), jnp.float32),
            pltpu.VMEM((F, F), jnp.float32),
            pltpu.VMEM((2, F, F, 128), jnp.float32),
            dma((6,)), dma((chunks,)), dma((chunks,)), dma((chunks,)), dma((chunks,)), dma((chunks,)), dma((chunks,)),
            dma, dma, dma, regular, regular, regular,
            dma((chunks,)), regular,
        ],
        compiler_params=pltpu.CompilerParams(
            collective_id=0, has_side_effects=True, vmem_limit_bytes=40 * 1024 * 1024
        ),
    )(*arrays)
    return pl.pallas_call(
        put_out,
        out_shape=tuple(pltpu.HBM(shape, jnp.float32) for shape in shapes),
        in_specs=[pl.BlockSpec(memory_space=pltpu.VMEM)] * 2,
        out_specs=(pl.BlockSpec(memory_space=pltpu.HBM),) * 2,
        scratch_shapes=[pltpu.SemaphoreType.DMA((PARTS + 1,))],
        compiler_params=pltpu.CompilerParams(vmem_limit_bytes=1024 * 1024),
    )(*results)


def solution(mesh):
    groups, members = mesh.shape["grp"], mesh.shape["dev"]
    return jax.shard_map(
        functools.partial(per_device, groups, members),
        mesh=mesh,
        in_specs=(P(None, ("grp", "dev"), None, None), P(), P()),
        out_specs=(P(None, ("grp", "dev"), None, None), P(None, "grp", "dev", None)),
        check_vma=False,
    )
```

```python
import functools

import jax
import jax.numpy as jnp
from jax import lax
from jax.experimental import pallas as pl
from jax.experimental.pallas import tpu as pltpu
from jax.sharding import PartitionSpec as P

MESH = pl.DeviceIdType.MESH
F = 24
HALF = 12
ROWS = 8
LAG = 8
PIECES = 1
HOLD_P = 1
HOLD_R = 2
HOLD_D = 4
HOLD_V = 5
PARTS = 8
AHEAD = 20
TURN_END = 24
EVERY = 8
HOLD_F = 3
BLOCK = 12
COMPUTE = True
WEYL = True


def d12(m2, m1, p1, p2):
    return 8.0 * (p1 - m1) - (p2 - m2)


def kernel(groups, members, fields, mix_in, lap_in, rhs, weyl, own, halo, via, tsum, w1, w2, wl,
           mix, lapw, wrow, load_sem, send_p, recv_p, send_r, recv_r, send_d, recv_d, wsend, wrecv, wlocal,
           up, far, ready, send_f, over):
    depth = fields.shape[1]
    rows = fields.shape[2]
    width = fields.shape[3]
    tiles = rows // ROWS
    steps = 2 * tiles
    share = rows // members
    g = lax.axis_index("grp")
    d = lax.axis_index("dev")
    slabs = groups * members
    s = g * members + d
    odd = lax.rem(d, 2)
    partner = d + 1 - 2 * odd
    target = lax.rem(s + 2 - 4 * odd + slabs, slabs)
    target_id = {"grp": target // members, "dev": lax.rem(target, members)}
    end = members - 1
    godd = lax.rem(g, 2)

    def group(by):
        return {"grp": lax.rem(g + by + groups, groups)}

    hub = ((godd == 1) & (d == end - 1)) | ((godd == 0) & (d == 1))
    direct = ((godd == 1) & (d == end)) | ((godd == 0) & (d == 0))
    relays = jnp.logical_not(hub)
    hub_id = {"grp": lax.rem(g + 1 - 2 * godd + groups, groups), "dev": jnp.where(d == 0, end - 1, 1)}
    hub_target = {**group(2), "dev": jnp.where(d == 1, 0, end)}

    low, high = pl.ds(0, HALF), pl.ds(HALF, HALF)
    opening = pltpu.make_async_copy(
        fields.at[low, :, pl.ds(0, ROWS), :], own.at[low, :, pl.ds(8, ROWS), :], load_sem.at[6])
    opening.start()
    loads = [pltpu.make_async_copy(
        fields.at[low, :, pl.ds(ROWS, rows - ROWS), :],
        own.at[low, :, pl.ds(8 + ROWS, rows - ROWS), :], load_sem.at[0])]
    loads.append(pltpu.make_async_copy(
        fields.at[high], own.at[high, :, pl.ds(8, rows), :], load_sem.at[1]))
    loads.append(pltpu.make_async_copy(
        fields.at[:, :, pl.ds(rows - 8, 8), :], own.at[:, :, pl.ds(0, 8), :], load_sem.at[2]))
    loads.append(pltpu.make_async_copy(
        fields.at[:, :, pl.ds(0, 8), :], own.at[:, :, pl.ds(rows + 8, 8), :], load_sem.at[3]))
    loads.append(pltpu.make_async_copy(mix_in, mix, load_sem.at[4]))
    loads.append(pltpu.make_async_copy(lap_in, lapw, load_sem.at[5]))
    for load in loads:
        load.start()

    barrier = pltpu.get_barrier_semaphore()

    def hello(to):
        pl.semaphore_signal(barrier, inc=1, device_id=to, device_id_type=MESH)

    def greet(to, _):
        hello({"dev": to})
        return 0

    @pl.when(odd == 1)
    def _():
        hello({"dev": d - 1})

    lax.fori_loop(d + 1, members, greet, 0)

    @pl.when((d == 0) & (godd == 1))
    def _():
        hello({**group(-1), "dev": end - 1})

    @pl.when((d == 1) & (godd == 1))
    def _():
        hello({**group(-1), "dev": end})

    @pl.when((d == 0) & (godd == 0))
    def _():
        hello({**group(1), "dev": end - 1})
        hello({**group(2), "dev": 1})

    @pl.when((d == 1) & (godd == 0))
    def _():
        hello({**group(1), "dev": end})

    @pl.when((d == end) & (godd == 1))
    def _():
        hello({**group(2), "dev": end - 1})

    wide = ((odd == 0) & (d <= end - 3)) | ((odd == 1) & (d >= 3))

    @pl.when((odd == 0) & (d <= end - 3))
    def _():
        hello({**group(2), "dev": d + 3})

    @pl.when((odd == 0) & (d >= 2))
    def _():
        hello({**group(2), "dev": d + 1})

    @pl.when((odd == 1) & (d < end))
    def _():
        hello({**group(2), "dev": d - 1})

    wider = jnp.where(wide, 1 + odd, 0)
    extra = wider + jnp.where(d == end, 1, jnp.where(d == end - 1, 1 + godd, jnp.where(d == 1, 1 - godd, 0)))
    pl.semaphore_wait(barrier, d + (1 - odd) + extra)

    size = HALF // PIECES
    last = PIECES + steps - 2

    def window(k, kind):
        if kind == 0:
            return pl.ds(k * size, size), 0
        if kind == 2:
            return pl.ds(HALF + (k - last) * size, size), rows - ROWS
        part = k - (PIECES - 1)
        return pl.ds((part // tiles) * HALF, HALF), pl.multiple_of(lax.rem(part, tiles) * ROWS, ROWS)

    def run(kind, first, stop, body):
        def once(k, _):
            body(k, kind)
            return 0
        lax.fori_loop(first, stop, once, 0)

    def each(body, low=0, high=steps):
        if low == 0:
            run(0, 0, PIECES, body)
        run(1, max(low, 1) + PIECES - 1, min(high, steps - 1) + PIECES - 1, body)
        if high == steps:
            run(2, last, last + PIECES, body)

    def at(part, body):
        @pl.when(part == 0)
        def _():
            run(0, 0, PIECES, body)

        @pl.when((part > 0) & (part < steps - 1))
        def _():
            body(part + PIECES - 1, 1)

        @pl.when(part == steps - 1)
        def _():
            run(2, last, last + PIECES, body)

    def own_chunk(k, kind):
        part, r0 = window(k, kind)
        return own.at[part, :, pl.ds(r0 + 8, ROWS), :]

    def halo_chunk(slot, k, kind):
        part, r0 = window(k, kind)
        return halo.at[slot, part, :, pl.ds(r0, ROWS), :]

    def via_chunk(k, kind):
        part, r0 = window(k, kind)
        return via.at[part, :, pl.ds(r0, ROWS), :]

    mine = 1 - odd

    def to_partner(k, kind):
        return pltpu.make_async_remote_copy(
            own_chunk(k, kind), halo_chunk(odd, k, kind), send_p.at[k], recv_p.at[k],
            device_id={"dev": partner}, device_id_type=MESH)

    def relay(k, kind):
        return pltpu.make_async_remote_copy(
            halo_chunk(mine, k, kind), halo_chunk(odd, k, kind), send_r.at[k], recv_r.at[k],
            device_id=target_id, device_id_type=MESH)

    def straight(k, kind):
        return pltpu.make_async_remote_copy(
            own_chunk(k, kind), via_chunk(k, kind), send_d.at[k], recv_d.at[k],
            device_id=hub_id, device_id_type=MESH)

    def hand_on(k, kind):
        return pltpu.make_async_remote_copy(
            via_chunk(k, kind), halo_chunk(mine, k, kind), send_r.at[k], recv_r.at[k],
            device_id=hub_target, device_id_type=MESH)

    def detour(k, kind):
        return pltpu.make_async_remote_copy(
            halo_chunk(mine, k, kind), via_chunk(k, kind), send_r.at[k], recv_d.at[k],
            device_id={**group(2), "dev": d + 3 - 6 * odd}, device_id_type=MESH)

    def hand_back(k, kind):
        return pltpu.make_async_remote_copy(
            via_chunk(k, kind), halo_chunk(mine, k, kind), send_f.at[k], recv_r.at[k],
            device_id={**group(2), "dev": partner}, device_id_type=MESH)

    def turn(part):
        return wide & (part > 0) & (part < TURN_END) & (lax.rem(part, EVERY) == EVERY - 1)

    def send(k, kind):
        to_partner(k, kind).start()

    def send_straight(k, kind):
        straight(k, kind).start()

    yields = (d == end) & (godd == 1)

    opening.wait()

    @pl.when(jnp.logical_not(yields))
    def _():
        each(send, 0, 1)

    loads[0].wait()

    @pl.when(jnp.logical_not(yields))
    def _():
        each(send, 1, min(AHEAD, tiles))

    @pl.when((odd == 0) & (d >= 2))
    def _():
        pl.semaphore_signal(up, inc=1, device_id={"dev": d - 2}, device_id_type=MESH)

    @pl.when((odd == 1) & (d >= 3))
    def _():
        pl.semaphore_signal(over, inc=1, device_id={**group(2), "dev": d - 3}, device_id_type=MESH)

    @pl.when((d == end) & (godd == 0))
    def _():
        pl.semaphore_signal(up, inc=1, device_id={**group(1), "dev": 1}, device_id_type=MESH)

    @pl.when((d == end - 1) & (godd == 1))
    def _():
        pl.semaphore_signal(far, inc=1, device_id={**group(-1), "dev": 0}, device_id_type=MESH)

    loads[1].wait()

    if AHEAD > tiles:
        @pl.when(jnp.logical_not(yields))
        def _():
            each(send, tiles, AHEAD)

    @pl.when(yields)
    def _():
        each(send_straight)

    def reply(to, _):
        pl.semaphore_signal(ready, inc=1, device_id={"dev": to}, device_id_type=MESH)
        return 0

    lax.fori_loop(0, d, reply, 0)
    loads[2].wait()
    loads[3].wait()

    loads[4].wait()
    loads[5].wait()
    if COMPUTE:
        lap_all = lapw[...]
        for slot, table in enumerate((mix[...] - 7.5 * lap_all, lap_all * (1.0 / 12.0))):
            for h in range(F):
                wrow[slot, h] = jnp.broadcast_to(table[:, h:h + 1], (F, 128))

        def spread(h, _):
            for slot, into in enumerate((w1, w2)):
                for c in range(F):
                    into[h, c] = jnp.broadcast_to(wrow[slot, h, c:c + 1, :], (8, 128))
            return 0

        lax.fori_loop(0, F, spread, 0)

    lane = lax.broadcasted_iota(jnp.int32, (ROWS, width), 1).astype(jnp.float32)
    line = lax.broadcasted_iota(jnp.int32, (ROWS, width), 0).astype(jnp.float32)

    def near(h, r0, p, halos=True):
        def along(off):
            return own[h, p, pl.ds(r0 + 8 + off, ROWS), :]
        mid = pl.ds(pl.multiple_of(r0 + 8, 8), ROWS)
        here = own[h, p, mid, :]
        rows_at = pl.ds(pl.multiple_of(r0, 8), ROWS)
        xs = [pltpu.roll(here, 2, 1), pltpu.roll(here, 1, 1),
              pltpu.roll(here, width - 1, 1), pltpu.roll(here, width - 2, 1)]
        ys = [along(-2), along(-1), along(1), along(2)]
        other = own[h, 1 - p, mid, :]
        if not halos:
            return here, xs, ys, other
        if p == 0:
            zs = [halo[0, h, 0, rows_at, :], halo[0, h, 1, rows_at, :],
                  other, halo[1, h, 0, rows_at, :]]
        else:
            zs = [halo[0, h, 1, rows_at, :], other,
                  halo[1, h, 0, rows_at, :], halo[1, h, 1, rows_at, :]]
        return here, xs, ys, zs

    def lap_sum(xs, ys, zs):
        one = (xs[1] + xs[2]) + (ys[1] + ys[2]) + (zs[1] + zs[2])
        two = (xs[0] + xs[3]) + (ys[0] + ys[3]) + (zs[0] + zs[3])
        return 16.0 * one - two

    def weyl_tile(tile):
        r0 = tile * ROWS
        xpos = lane + (0.5 - 0.5 * width)
        ypos = line + (r0.astype(jnp.float32) + (0.5 - 0.5 * rows))
        sq = xpos * xpos + ypos * ypos
        inv_s = lax.rsqrt(sq)
        cyl = sq * inv_s
        cosp = xpos * inv_s
        sinp = ypos * inv_s
        for p in range(depth):
            zpos = (s * depth + p).astype(jnp.float32) + (0.5 - 0.5 * slabs * depth)
            inv_r = lax.rsqrt(sq + zpos * zpos)
            zr = zpos * inv_r
            theta = (zr * cosp, zr * sinp, -(cyl * inv_r))
            phi = (-sinp, cosp)
            curv = []
            grad = []
            for h in range(6, 12):
                here, xs, ys, zs = near(h, r0, p)
                curv.append(here)
                grad.append((d12(*xs), d12(*ys), d12(*zs)))
            trace = curv[0] + curv[3] + curv[5]
            table = ((0, 1, 2), (1, 3, 4), (2, 4, 5))
            pairs = ((0, 0), (0, 1), (0, 2), (1, 1), (1, 2), (2, 2))

            def curl(i, j):
                n1, n2 = (i + 1) % 3, (i + 2) % 3
                return grad[table[n2][j]][n1] - grad[table[n1][j]][n2]

            real = None
            imag = None
            for comp, (i, j) in enumerate(pairs):
                here, xs, ys, zs = near(comp, r0, p)
                lap = lap_sum(xs, ys, zs) - 90.0 * here
                elec = lap * (-0.5 / 12.0) - trace * curv[comp]
                for m in range(3):
                    elec = elec + curv[table[i][m]] * curv[table[m][j]]
                if i == j:
                    mag = curl(i, i) * (1.0 / 12.0)
                else:
                    mag = (curl(i, j) + curl(j, i)) * (0.5 / 12.0)
                fi = phi[i] if i < 2 else None
                fj = phi[j] if j < 2 else None
                tt = theta[i] * theta[j]
                both = tt if fi is None or fj is None else tt - fi * fj
                mixed = None
                for u, v in ((theta[i], fj), (theta[j], fi)):
                    if v is not None:
                        mixed = u * v if mixed is None else mixed + u * v
                if i == j:
                    both = 0.5 * both
                    mixed = None if mixed is None else 0.5 * mixed
                one = elec * both
                two = mag * both
                if mixed is not None:
                    one = one - mag * mixed
                    two = two + elec * mixed
                real = one if real is None else real + one
                imag = two if imag is None else imag + two
            imag = -imag
            per = ROWS // share
            for k in range(per):
                wl[tile * per + k, 0, p] = real[k * share:(k + 1) * share]
                wl[tile * per + k, 1, p] = imag[k * share:(k + 1) * share]

    def weyl_send(tile):
        per = ROWS // share
        for k in range(per):
            to = tile * per + k

            @pl.when(to == d)
            def _():
                pltpu.make_async_copy(
                    wl.at[to], weyl.at[:, pl.ds(d * depth, depth)], wlocal).start()

            @pl.when(to != d)
            def _():
                pltpu.make_async_remote_copy(
                    wl.at[to], weyl.at[:, pl.ds(d * depth, depth)], wsend, wrecv,
                    device_id={"dev": to}, device_id_type=MESH).start()

    def mixed(tile, h0, h1, with_own):
        mid = pl.ds(pl.multiple_of(tile * ROWS + 8, 8), ROWS)
        out = pl.ds(pl.multiple_of(tile * ROWS, 8), ROWS)
        for c0 in range(0, F, BLOCK):
            def mixing(h4, acc):
                for k in range(4):
                    h = h4 * 4 + k
                    if with_own:
                        acc = acc + w1[h, pl.ds(c0, BLOCK)][:, None] * own[h, :, mid, :][None]
                    acc = acc + w2[h, pl.ds(c0, BLOCK)][:, None] * tsum[h][None]
                return acc
            start = rhs[pl.ds(c0, BLOCK), :, out, :]
            rhs[pl.ds(c0, BLOCK), :, out, :] = lax.fori_loop(h0 // 4, h1 // 4, mixing, start)

    def rhs_early(tile):
        r0 = tile * ROWS
        mid = pl.ds(pl.multiple_of(r0 + 8, 8), ROWS)
        out = pl.ds(pl.multiple_of(r0, 8), ROWS)

        def stencil(halos, h4, _):
            for p in range(depth):
                bz = own[12, p, mid, :] * (1.0 / 12.0)
                by = own[13, p, mid, :] * (1.0 / 12.0)
                bx = own[14, p, mid, :] * (1.0 / 12.0)
                for k in range(4):
                    h = h4 * 4 + k
                    here, xs, ys, zs = near(h, r0, p, halos)
                    if halos:
                        tsum[h, p] = lap_sum(xs, ys, zs)
                        dz = d12(*zs)
                    else:
                        one = (xs[1] + xs[2]) + (ys[1] + ys[2]) + zs
                        two = (xs[0] + xs[3]) + (ys[0] + ys[3])
                        tsum[h, p] = 16.0 * one - two
                        dz = (8.0 if p == 0 else -8.0) * zs
                    rhs[h, p, out, :] = bx * d12(*xs) + by * d12(*ys) + bz * dz
            return 0

        lax.fori_loop(0, HALF // 4, functools.partial(stencil, True), 0)
        lax.fori_loop(HALF // 4, F // 4, functools.partial(stencil, False), 0)
        mixed(tile, 0, F, True)

    def rhs_late(tile):
        r0 = tile * ROWS
        mid = pl.ds(pl.multiple_of(r0 + 8, 8), ROWS)
        out = pl.ds(pl.multiple_of(r0, 8), ROWS)

        def planes(h4, _):
            for p in range(depth):
                bz = own[12, p, mid, :] * (1.0 / 12.0)
                for k in range(4):
                    h = h4 * 4 + k
                    below = halo[0, h, 1, out, :]
                    above = halo[1, h, 0, out, :]
                    if p == 0:
                        far = halo[0, h, 0, out, :]
                        tsum[h, p] = 16.0 * below - (far + above)
                        dz = (far - above) - 8.0 * below
                    else:
                        far = halo[1, h, 1, out, :]
                        tsum[h, p] = 16.0 * above - (below + far)
                        dz = 8.0 * above + (below - far)
                    rhs[h, p, out, :] = rhs[h, p, out, :] + bz * dz
            return 0

        lax.fori_loop(HALF // 4, F // 4, planes, 0)
        mixed(tile, HALF, F, False)

    asks = ((odd == 0) & (d < end - 1)) | ((d == 1) & (godd == 1))
    held = (d == 1) & (godd == 1)
    hold_hub = jnp.where(d == 1, HOLD_V, 1)

    def ask():
        @pl.when(asks)
        def _():
            pl.semaphore_wait(up, 1)

    def arrived(k, kind):
        to_partner(k, kind).wait_recv()
        if kind == 1:
            astray = turn(k - (PIECES - 1))

            @pl.when(astray)
            def _():
                detour(k, kind).start()

            @pl.when(relays & jnp.logical_not(held | astray))
            def _():
                relay(k, kind).start()
        else:
            @pl.when(relays & jnp.logical_not(held))
            def _():
                relay(k, kind).start()

    def late_relay(k, kind):
        relay(k, kind).start()

    def pass_on(k, kind):
        straight(k, kind).wait_recv()
        hand_on(k, kind).start()

    def done(k, kind):
        relay(k, kind).wait_recv()
        to_partner(k, kind).wait_send()
        relay(k, kind).wait_send()
        if kind == 1:
            @pl.when(turn(k - (PIECES - 1)))
            def _():
                hand_back(k, kind).wait_send()

        @pl.when(direct)
        def _():
            straight(k, kind).wait_send()

    def passed(part):
        return jnp.minimum(jnp.minimum(jnp.maximum(2 * (part - hold_hub), 0), part), steps)

    def step(part, _):
        @pl.when((part == 0) & jnp.logical_not(held))
        def _():
            ask()

        @pl.when((part == EVERY - 1) & wide & (odd == 0))
        def _():
            pl.semaphore_wait(over, 1)

        at(part, arrived)

        @pl.when(turn(part - HOLD_F))
        def _():
            k = part - HOLD_F + PIECES - 1
            straight(k, 1).wait_recv()
            hand_back(k, 1).start()

        @pl.when(held)
        def _():
            @pl.when(part == HOLD_R)
            def _():
                ask()
            at(part - HOLD_R, late_relay)

        @pl.when(yields & (part == HOLD_P))
        def _():
            each(send, 0, AHEAD + HOLD_P)

        @pl.when(jnp.logical_not(yields & (part < HOLD_P)))
        def _():
            at(part + AHEAD, send)

        @pl.when(direct & (d == 0) & (part == HOLD_D))
        def _():
            pl.semaphore_wait(far, 1)
            each(send_straight)

        @pl.when(hub)
        def _():
            def catch_up(v, _):
                at(v, pass_on)
                return 0
            lax.fori_loop(passed(part), passed(part + 1), catch_up, 0)

        j = part - LAG
        at(j, done)

        @pl.when((j == 1) & (d < end))
        def _():
            pl.semaphore_wait(ready, end - d)

        if WEYL:
            @pl.when((j >= 1) & (j <= tiles))
            def _():
                weyl_send(j - 1)

        if COMPUTE:
            @pl.when((j >= 0) & (j < tiles))
            def _():
                weyl_tile(j)
                rhs_early(j)

            @pl.when(j >= tiles)
            def _():
                rhs_late(j - tiles)
        return 0

    lax.fori_loop(0, steps + LAG, step, 0)

    if WEYL:
        sent = wl.at[pl.ds(0, members - 1)]
        pltpu.make_async_copy(sent, sent, wsend).wait()
        came = weyl.at[:, pl.ds(0, depth * (members - 1))]
        pltpu.make_async_copy(came, came, wrecv).wait()
        pltpu.make_async_copy(wl.at[0], weyl.at[:, pl.ds(0, depth)], wlocal).wait()


def put_out(rhs_in, weyl_in, rhs, weyl, sem):
    each = F // PARTS
    copies = [pltpu.make_async_copy(weyl_in, weyl, sem.at[PARTS])]
    for k in range(PARTS):
        part = pl.ds(k * each, each)
        copies.append(pltpu.make_async_copy(rhs_in.at[part], rhs.at[part], sem.at[k]))
    for copy in copies:
        copy.start()
    for copy in copies:
        copy.wait()


def per_device(groups, members, fields, mix_matrix, laplace_matrix):
    depth, rows, width = fields.shape[1:]
    share = rows // members
    chunks = 2 * (rows // ROWS) - 2 + 2 * PIECES
    arrays = [pltpu.with_memory_space_constraint(a, pltpu.HBM)
              for a in (fields, mix_matrix, laplace_matrix)]
    dma = pltpu.SemaphoreType.DMA
    regular = pltpu.SemaphoreType.REGULAR
    shapes = (fields.shape, (2, depth * members, share, width))
    results = pl.pallas_call(
        functools.partial(kernel, groups, members),
        out_shape=tuple(pltpu.VMEM(shape, jnp.float32) for shape in shapes),
        in_specs=[
            pl.BlockSpec(memory_space=pltpu.HBM),
            pl.BlockSpec(memory_space=pltpu.HBM),
            pl.BlockSpec(memory_space=pltpu.HBM),
        ],
        out_specs=(pl.BlockSpec(memory_space=pltpu.VMEM), pl.BlockSpec(memory_space=pl.ANY)),
        scratch_shapes=[
            pltpu.VMEM((F, depth, rows + 16, width), jnp.float32),
            pltpu.VMEM((2, F, depth, rows, width), jnp.float32),
            pltpu.VMEM((F, depth, rows, width), jnp.float32),
            pltpu.VMEM((F, depth, ROWS, width), jnp.float32),
            pltpu.VMEM((F, F, 8, 128), jnp.float32),
            pltpu.VMEM((F, F, 8, 128), jnp.float32),
            pltpu.VMEM((members, 2, depth, share, width), jnp.float32),
            pltpu.VMEM((F, F), jnp.float32),
            pltpu.VMEM((F, F), jnp.float32),
            pltpu.VMEM((2, F, F, 128), jnp.float32),
            dma((7,)), dma((chunks,)), dma((chunks,)), dma((chunks,)), dma((chunks,)), dma((chunks,)), dma((chunks,)),
            dma, dma, dma, regular, regular, regular,
            dma((chunks,)), regular,
        ],
        compiler_params=pltpu.CompilerParams(
            collective_id=0, has_side_effects=True, vmem_limit_bytes=40 * 1024 * 1024
        ),
    )(*arrays)
    return pl.pallas_call(
        put_out,
        out_shape=tuple(pltpu.HBM(shape, jnp.float32) for shape in shapes),
        in_specs=[pl.BlockSpec(memory_space=pltpu.VMEM)] * 2,
        out_specs=(pl.BlockSpec(memory_space=pltpu.HBM),) * 2,
        scratch_shapes=[pltpu.SemaphoreType.DMA((PARTS + 1,))],
        compiler_params=pltpu.CompilerParams(vmem_limit_bytes=1024 * 1024),
    )(*results)


def solution(mesh):
    groups, members = mesh.shape["grp"], mesh.shape["dev"]
    return jax.shard_map(
        functools.partial(per_device, groups, members),
        mesh=mesh,
        in_specs=(P(None, ("grp", "dev"), None, None), P(), P()),
        out_specs=(P(None, ("grp", "dev"), None, None), P(None, "grp", "dev", None)),
        check_vma=False,
    )
```

```python
import functools

import jax
import jax.numpy as jnp
from jax import lax
from jax.experimental import pallas as pl
from jax.experimental.pallas import tpu as pltpu
from jax.sharding import PartitionSpec as P

MESH = pl.DeviceIdType.MESH
F = 24
HALF = 12
ROWS = 8
LAG = 8
PIECES = 1
HOLD_P = 1
HOLD_R = 2
HOLD_D = 4
HOLD_V = 5
PARTS = 4
AHEAD = 20
TURN_END = 24
EVERY = 8
HOLD_F = 3
BLOCK = 12
COMPUTE = True
WEYL = True


def d12(m2, m1, p1, p2):
    return 8.0 * (p1 - m1) - (p2 - m2)


def kernel(groups, members, fields, mix_in, lap_in, rhs, weyl, own, halo, via, tsum, w1, w2, wl,
           mix, lapw, wrow, load_sem, send_p, recv_p, send_r, recv_r, send_d, recv_d, wsend, wrecv, wlocal,
           up, far, ready, send_f, over):
    depth = fields.shape[1]
    rows = fields.shape[2]
    width = fields.shape[3]
    tiles = rows // ROWS
    steps = 2 * tiles
    share = rows // members
    g = lax.axis_index("grp")
    d = lax.axis_index("dev")
    slabs = groups * members
    s = g * members + d
    odd = lax.rem(d, 2)
    partner = d + 1 - 2 * odd
    target = lax.rem(s + 2 - 4 * odd + slabs, slabs)
    target_id = {"grp": target // members, "dev": lax.rem(target, members)}
    end = members - 1
    godd = lax.rem(g, 2)

    def group(by):
        return {"grp": lax.rem(g + by + groups, groups)}

    hub = ((godd == 1) & (d == end - 1)) | ((godd == 0) & (d == 1))
    direct = ((godd == 1) & (d == end)) | ((godd == 0) & (d == 0))
    relays = jnp.logical_not(hub)
    hub_id = {"grp": lax.rem(g + 1 - 2 * godd + groups, groups), "dev": jnp.where(d == 0, end - 1, 1)}
    hub_target = {**group(2), "dev": jnp.where(d == 1, 0, end)}

    low, high = pl.ds(0, HALF), pl.ds(HALF, HALF)
    opening = pltpu.make_async_copy(
        fields.at[low, :, pl.ds(0, ROWS), :], own.at[low, :, pl.ds(8, ROWS), :], load_sem.at[6])
    opening.start()
    loads = [pltpu.make_async_copy(
        fields.at[low, :, pl.ds(ROWS, rows - ROWS), :],
        own.at[low, :, pl.ds(8 + ROWS, rows - ROWS), :], load_sem.at[0])]
    loads.append(pltpu.make_async_copy(
        fields.at[high], own.at[high, :, pl.ds(8, rows), :], load_sem.at[1]))
    loads.append(pltpu.make_async_copy(
        fields.at[:, :, pl.ds(rows - 8, 8), :], own.at[:, :, pl.ds(0, 8), :], load_sem.at[2]))
    loads.append(pltpu.make_async_copy(
        fields.at[:, :, pl.ds(0, 8), :], own.at[:, :, pl.ds(rows + 8, 8), :], load_sem.at[3]))
    loads.append(pltpu.make_async_copy(mix_in, mix, load_sem.at[4]))
    loads.append(pltpu.make_async_copy(lap_in, lapw, load_sem.at[5]))
    for load in loads:
        load.start()

    barrier = pltpu.get_barrier_semaphore()

    def hello(to):
        pl.semaphore_signal(barrier, inc=1, device_id=to, device_id_type=MESH)

    def greet(to, _):
        hello({"dev": to})
        return 0

    @pl.when(odd == 1)
    def _():
        hello({"dev": d - 1})

    lax.fori_loop(d + 1, members, greet, 0)

    @pl.when((d == 0) & (godd == 1))
    def _():
        hello({**group(-1), "dev": end - 1})

    @pl.when((d == 1) & (godd == 1))
    def _():
        hello({**group(-1), "dev": end})

    @pl.when((d == 0) & (godd == 0))
    def _():
        hello({**group(1), "dev": end - 1})
        hello({**group(2), "dev": 1})

    @pl.when((d == 1) & (godd == 0))
    def _():
        hello({**group(1), "dev": end})

    @pl.when((d == end) & (godd == 1))
    def _():
        hello({**group(2), "dev": end - 1})

    wide = ((odd == 0) & (d <= end - 3)) | ((odd == 1) & (d >= 3))

    @pl.when((odd == 0) & (d <= end - 3))
    def _():
        hello({**group(2), "dev": d + 3})

    @pl.when((odd == 0) & (d >= 2))
    def _():
        hello({**group(2), "dev": d + 1})

    @pl.when((odd == 1) & (d < end))
    def _():
        hello({**group(2), "dev": d - 1})

    wider = jnp.where(wide, 1 + odd, 0)
    extra = wider + jnp.where(d == end, 1, jnp.where(d == end - 1, 1 + godd, jnp.where(d == 1, 1 - godd, 0)))
    pl.semaphore_wait(barrier, d + (1 - odd) + extra)

    size = HALF // PIECES
    last = PIECES + steps - 2

    def window(k, kind):
        if kind == 0:
            return pl.ds(k * size, size), 0
        if kind == 2:
            return pl.ds(HALF + (k - last) * size, size), rows - ROWS
        part = k - (PIECES - 1)
        return pl.ds((part // tiles) * HALF, HALF), pl.multiple_of(lax.rem(part, tiles) * ROWS, ROWS)

    def run(kind, first, stop, body):
        def once(k, _):
            body(k, kind)
            return 0
        lax.fori_loop(first, stop, once, 0)

    def each(body, low=0, high=steps):
        if low == 0:
            run(0, 0, PIECES, body)
        run(1, max(low, 1) + PIECES - 1, min(high, steps - 1) + PIECES - 1, body)
        if high == steps:
            run(2, last, last + PIECES, body)

    def at(part, body):
        @pl.when(part == 0)
        def _():
            run(0, 0, PIECES, body)

        @pl.when((part > 0) & (part < steps - 1))
        def _():
            body(part + PIECES - 1, 1)

        @pl.when(part == steps - 1)
        def _():
            run(2, last, last + PIECES, body)

    def own_chunk(k, kind):
        part, r0 = window(k, kind)
        return own.at[part, :, pl.ds(r0 + 8, ROWS), :]

    def halo_chunk(slot, k, kind):
        part, r0 = window(k, kind)
        return halo.at[slot, part, :, pl.ds(r0, ROWS), :]

    def via_chunk(k, kind):
        part, r0 = window(k, kind)
        return via.at[part, :, pl.ds(r0, ROWS), :]

    mine = 1 - odd

    def to_partner(k, kind):
        return pltpu.make_async_remote_copy(
            own_chunk(k, kind), halo_chunk(odd, k, kind), send_p.at[k], recv_p.at[k],
            device_id={"dev": partner}, device_id_type=MESH)

    def relay(k, kind):
        return pltpu.make_async_remote_copy(
            halo_chunk(mine, k, kind), halo_chunk(odd, k, kind), send_r.at[k], recv_r.at[k],
            device_id=target_id, device_id_type=MESH)

    def straight(k, kind):
        return pltpu.make_async_remote_copy(
            own_chunk(k, kind), via_chunk(k, kind), send_d.at[k], recv_d.at[k],
            device_id=hub_id, device_id_type=MESH)

    def hand_on(k, kind):
        return pltpu.make_async_remote_copy(
            via_chunk(k, kind), halo_chunk(mine, k, kind), send_r.at[k], recv_r.at[k],
            device_id=hub_target, device_id_type=MESH)

    def detour(k, kind):
        return pltpu.make_async_remote_copy(
            halo_chunk(mine, k, kind), via_chunk(k, kind), send_r.at[k], recv_d.at[k],
            device_id={**group(2), "dev": d + 3 - 6 * odd}, device_id_type=MESH)

    def hand_back(k, kind):
        return pltpu.make_async_remote_copy(
            via_chunk(k, kind), halo_chunk(mine, k, kind), send_f.at[k], recv_r.at[k],
            device_id={**group(2), "dev": partner}, device_id_type=MESH)

    def turn(part):
        return wide & (part > 0) & (part < TURN_END) & (lax.rem(part, EVERY) == EVERY - 1)

    def send(k, kind):
        to_partner(k, kind).start()

    def send_straight(k, kind):
        straight(k, kind).start()

    yields = (d == end) & (godd == 1)

    opening.wait()

    @pl.when(jnp.logical_not(yields))
    def _():
        each(send, 0, 1)

    loads[0].wait()

    @pl.when(jnp.logical_not(yields))
    def _():
        each(send, 1, min(AHEAD, tiles))

    @pl.when((odd == 0) & (d >= 2))
    def _():
        pl.semaphore_signal(up, inc=1, device_id={"dev": d - 2}, device_id_type=MESH)

    @pl.when((odd == 1) & (d >= 3))
    def _():
        pl.semaphore_signal(over, inc=1, device_id={**group(2), "dev": d - 3}, device_id_type=MESH)

    @pl.when((d == end) & (godd == 0))
    def _():
        pl.semaphore_signal(up, inc=1, device_id={**group(1), "dev": 1}, device_id_type=MESH)

    @pl.when((d == end - 1) & (godd == 1))
    def _():
        pl.semaphore_signal(far, inc=1, device_id={**group(-1), "dev": 0}, device_id_type=MESH)

    loads[1].wait()

    if AHEAD > tiles:
        @pl.when(jnp.logical_not(yields))
        def _():
            each(send, tiles, AHEAD)

    @pl.when(yields)
    def _():
        each(send_straight)

    def reply(to, _):
        pl.semaphore_signal(ready, inc=1, device_id={"dev": to}, device_id_type=MESH)
        return 0

    lax.fori_loop(0, d, reply, 0)
    loads[2].wait()
    loads[3].wait()

    loads[4].wait()
    loads[5].wait()
    if COMPUTE:
        lap_all = lapw[...]
        for slot, table in enumerate((mix[...] - 7.5 * lap_all, lap_all * (1.0 / 12.0))):
            for h in range(F):
                wrow[slot, h] = jnp.broadcast_to(table[:, h:h + 1], (F, 128))

        def spread(h, _):
            for slot, into in enumerate((w1, w2)):
                for c in range(F):
                    into[h, c] = jnp.broadcast_to(wrow[slot, h, c:c + 1, :], (8, 128))
            return 0

        lax.fori_loop(0, F, spread, 0)

    lane = lax.broadcasted_iota(jnp.int32, (ROWS, width), 1).astype(jnp.float32)
    line = lax.broadcasted_iota(jnp.int32, (ROWS, width), 0).astype(jnp.float32)

    def near(h, r0, p, halos=True):
        def along(off):
            return own[h, p, pl.ds(r0 + 8 + off, ROWS), :]
        mid = pl.ds(pl.multiple_of(r0 + 8, 8), ROWS)
        here = own[h, p, mid, :]
        rows_at = pl.ds(pl.multiple_of(r0, 8), ROWS)
        xs = [pltpu.roll(here, 2, 1), pltpu.roll(here, 1, 1),
              pltpu.roll(here, width - 1, 1), pltpu.roll(here, width - 2, 1)]
        ys = [along(-2), along(-1), along(1), along(2)]
        other = own[h, 1 - p, mid, :]
        if not halos:
            return here, xs, ys, other
        if p == 0:
            zs = [halo[0, h, 0, rows_at, :], halo[0, h, 1, rows_at, :],
                  other, halo[1, h, 0, rows_at, :]]
        else:
            zs = [halo[0, h, 1, rows_at, :], other,
                  halo[1, h, 0, rows_at, :], halo[1, h, 1, rows_at, :]]
        return here, xs, ys, zs

    def lap_sum(xs, ys, zs):
        one = (xs[1] + xs[2]) + (ys[1] + ys[2]) + (zs[1] + zs[2])
        two = (xs[0] + xs[3]) + (ys[0] + ys[3]) + (zs[0] + zs[3])
        return 16.0 * one - two

    def weyl_tile(tile):
        r0 = tile * ROWS
        xpos = lane + (0.5 - 0.5 * width)
        ypos = line + (r0.astype(jnp.float32) + (0.5 - 0.5 * rows))
        sq = xpos * xpos + ypos * ypos
        inv_s = lax.rsqrt(sq)
        cyl = sq * inv_s
        cosp = xpos * inv_s
        sinp = ypos * inv_s
        for p in range(depth):
            zpos = (s * depth + p).astype(jnp.float32) + (0.5 - 0.5 * slabs * depth)
            inv_r = lax.rsqrt(sq + zpos * zpos)
            zr = zpos * inv_r
            theta = (zr * cosp, zr * sinp, -(cyl * inv_r))
            phi = (-sinp, cosp)
            curv = []
            grad = []
            for h in range(6, 12):
                here, xs, ys, zs = near(h, r0, p)
                curv.append(here)
                grad.append((d12(*xs), d12(*ys), d12(*zs)))
            trace = curv[0] + curv[3] + curv[5]
            table = ((0, 1, 2), (1, 3, 4), (2, 4, 5))
            pairs = ((0, 0), (0, 1), (0, 2), (1, 1), (1, 2), (2, 2))

            def curl(i, j):
                n1, n2 = (i + 1) % 3, (i + 2) % 3
                return grad[table[n2][j]][n1] - grad[table[n1][j]][n2]

            real = None
            imag = None
            for comp, (i, j) in enumerate(pairs):
                here, xs, ys, zs = near(comp, r0, p)
                lap = lap_sum(xs, ys, zs) - 90.0 * here
                elec = lap * (-0.5 / 12.0) - trace * curv[comp]
                for m in range(3):
                    elec = elec + curv[table[i][m]] * curv[table[m][j]]
                if i == j:
                    mag = curl(i, i) * (1.0 / 12.0)
                else:
                    mag = (curl(i, j) + curl(j, i)) * (0.5 / 12.0)
                fi = phi[i] if i < 2 else None
                fj = phi[j] if j < 2 else None
                tt = theta[i] * theta[j]
                both = tt if fi is None or fj is None else tt - fi * fj
                mixed = None
                for u, v in ((theta[i], fj), (theta[j], fi)):
                    if v is not None:
                        mixed = u * v if mixed is None else mixed + u * v
                if i == j:
                    both = 0.5 * both
                    mixed = None if mixed is None else 0.5 * mixed
                one = elec * both
                two = mag * both
                if mixed is not None:
                    one = one - mag * mixed
                    two = two + elec * mixed
                real = one if real is None else real + one
                imag = two if imag is None else imag + two
            imag = -imag
            per = ROWS // share
            for k in range(per):
                wl[tile * per + k, 0, p] = real[k * share:(k + 1) * share]
                wl[tile * per + k, 1, p] = imag[k * share:(k + 1) * share]

    def weyl_send(tile):
        per = ROWS // share
        for k in range(per):
            to = tile * per + k

            @pl.when(to == d)
            def _():
                pltpu.make_async_copy(
                    wl.at[to], weyl.at[:, pl.ds(d * depth, depth)], wlocal).start()

            @pl.when(to != d)
            def _():
                pltpu.make_async_remote_copy(
                    wl.at[to], weyl.at[:, pl.ds(d * depth, depth)], wsend, wrecv,
                    device_id={"dev": to}, device_id_type=MESH).start()

    def mixed(tile, h0, h1, with_own):
        mid = pl.ds(pl.multiple_of(tile * ROWS + 8, 8), ROWS)
        out = pl.ds(pl.multiple_of(tile * ROWS, 8), ROWS)
        for c0 in range(0, F, BLOCK):
            def mixing(h4, acc):
                for k in range(4):
                    h = h4 * 4 + k
                    if with_own:
                        acc = acc + w1[h, pl.ds(c0, BLOCK)][:, None] * own[h, :, mid, :][None]
                    acc = acc + w2[h, pl.ds(c0, BLOCK)][:, None] * tsum[h][None]
                return acc
            start = rhs[pl.ds(c0, BLOCK), :, out, :]
            rhs[pl.ds(c0, BLOCK), :, out, :] = lax.fori_loop(h0 // 4, h1 // 4, mixing, start)

    def rhs_early(tile):
        r0 = tile * ROWS
        mid = pl.ds(pl.multiple_of(r0 + 8, 8), ROWS)
        out = pl.ds(pl.multiple_of(r0, 8), ROWS)

        def stencil(halos, h4, _):
            for p in range(depth):
                bz = own[12, p, mid, :] * (1.0 / 12.0)
                by = own[13, p, mid, :] * (1.0 / 12.0)
                bx = own[14, p, mid, :] * (1.0 / 12.0)
                for k in range(4):
                    h = h4 * 4 + k
                    here, xs, ys, zs = near(h, r0, p, halos)
                    if halos:
                        tsum[h, p] = lap_sum(xs, ys, zs)
                        dz = d12(*zs)
                    else:
                        one = (xs[1] + xs[2]) + (ys[1] + ys[2]) + zs
                        two = (xs[0] + xs[3]) + (ys[0] + ys[3])
                        tsum[h, p] = 16.0 * one - two
                        dz = (8.0 if p == 0 else -8.0) * zs
                    rhs[h, p, out, :] = bx * d12(*xs) + by * d12(*ys) + bz * dz
            return 0

        lax.fori_loop(0, HALF // 4, functools.partial(stencil, True), 0)
        lax.fori_loop(HALF // 4, F // 4, functools.partial(stencil, False), 0)
        mixed(tile, 0, F, True)

    def rhs_late(tile):
        r0 = tile * ROWS
        mid = pl.ds(pl.multiple_of(r0 + 8, 8), ROWS)
        out = pl.ds(pl.multiple_of(r0, 8), ROWS)

        def planes(h4, _):
            for p in range(depth):
                bz = own[12, p, mid, :] * (1.0 / 12.0)
                for k in range(4):
                    h = h4 * 4 + k
                    below = halo[0, h, 1, out, :]
                    above = halo[1, h, 0, out, :]
                    if p == 0:
                        far = halo[0, h, 0, out, :]
                        tsum[h, p] = 16.0 * below - (far + above)
                        dz = (far - above) - 8.0 * below
                    else:
                        far = halo[1, h, 1, out, :]
                        tsum[h, p] = 16.0 * above - (below + far)
                        dz = 8.0 * above + (below - far)
                    rhs[h, p, out, :] = rhs[h, p, out, :] + bz * dz
            return 0

        lax.fori_loop(HALF // 4, F // 4, planes, 0)
        mixed(tile, HALF, F, False)

    asks = ((odd == 0) & (d < end - 1)) | ((d == 1) & (godd == 1))
    held = (d == 1) & (godd == 1)
    hold_hub = jnp.where(d == 1, HOLD_V, 1)

    def ask():
        @pl.when(asks)
        def _():
            pl.semaphore_wait(up, 1)

    def arrived(k, kind):
        to_partner(k, kind).wait_recv()
        if kind == 1:
            astray = turn(k - (PIECES - 1))

            @pl.when(astray)
            def _():
                detour(k, kind).start()

            @pl.when(relays & jnp.logical_not(held | astray))
            def _():
                relay(k, kind).start()
        else:
            @pl.when(relays & jnp.logical_not(held))
            def _():
                relay(k, kind).start()

    def late_relay(k, kind):
        relay(k, kind).start()

    def pass_on(k, kind):
        straight(k, kind).wait_recv()
        hand_on(k, kind).start()

    def done(k, kind):
        relay(k, kind).wait_recv()
        to_partner(k, kind).wait_send()
        relay(k, kind).wait_send()
        if kind == 1:
            @pl.when(turn(k - (PIECES - 1)))
            def _():
                hand_back(k, kind).wait_send()

        @pl.when(direct)
        def _():
            straight(k, kind).wait_send()

    def passed(part):
        return jnp.minimum(jnp.minimum(jnp.maximum(2 * (part - hold_hub), 0), part), steps)

    def step(part, _):
        @pl.when((part == 0) & jnp.logical_not(held))
        def _():
            ask()

        @pl.when((part == EVERY - 1) & wide & (odd == 0))
        def _():
            pl.semaphore_wait(over, 1)

        at(part, arrived)

        @pl.when(turn(part - HOLD_F))
        def _():
            k = part - HOLD_F + PIECES - 1
            straight(k, 1).wait_recv()
            hand_back(k, 1).start()

        @pl.when(held)
        def _():
            @pl.when(part == HOLD_R)
            def _():
                ask()
            at(part - HOLD_R, late_relay)

        @pl.when(yields & (part == HOLD_P))
        def _():
            each(send, 0, AHEAD + HOLD_P)

        @pl.when(jnp.logical_not(yields & (part < HOLD_P)))
        def _():
            at(part + AHEAD, send)

        @pl.when(direct & (d == 0) & (part == HOLD_D))
        def _():
            pl.semaphore_wait(far, 1)
            each(send_straight)

        @pl.when(hub)
        def _():
            def catch_up(v, _):
                at(v, pass_on)
                return 0
            lax.fori_loop(passed(part), passed(part + 1), catch_up, 0)

        j = part - LAG
        at(j, done)

        @pl.when((j == 1) & (d < end))
        def _():
            pl.semaphore_wait(ready, end - d)

        if WEYL:
            @pl.when((j >= 1) & (j <= tiles))
            def _():
                weyl_send(j - 1)

        if COMPUTE:
            @pl.when((j >= 0) & (j < tiles))
            def _():
                weyl_tile(j)
                rhs_early(j)

            @pl.when(j >= tiles)
            def _():
                rhs_late(j - tiles)
        return 0

    lax.fori_loop(0, steps + LAG, step, 0)

    if WEYL:
        sent = wl.at[pl.ds(0, members - 1)]
        pltpu.make_async_copy(sent, sent, wsend).wait()
        came = weyl.at[:, pl.ds(0, depth * (members - 1))]
        pltpu.make_async_copy(came, came, wrecv).wait()
        pltpu.make_async_copy(wl.at[0], weyl.at[:, pl.ds(0, depth)], wlocal).wait()


def put_out(rhs_in, weyl_in, rhs, weyl, sem):
    each = F // PARTS
    copies = [pltpu.make_async_copy(weyl_in, weyl, sem.at[PARTS])]
    for k in range(PARTS):
        part = pl.ds(k * each, each)
        copies.append(pltpu.make_async_copy(rhs_in.at[part], rhs.at[part], sem.at[k]))
    for copy in copies:
        copy.start()
    for copy in copies:
        copy.wait()


def per_device(groups, members, fields, mix_matrix, laplace_matrix):
    depth, rows, width = fields.shape[1:]
    share = rows // members
    chunks = 2 * (rows // ROWS) - 2 + 2 * PIECES
    arrays = [pltpu.with_memory_space_constraint(a, pltpu.HBM)
              for a in (fields, mix_matrix, laplace_matrix)]
    dma = pltpu.SemaphoreType.DMA
    regular = pltpu.SemaphoreType.REGULAR
    shapes = (fields.shape, (2, depth * members, share, width))
    results = pl.pallas_call(
        functools.partial(kernel, groups, members),
        out_shape=tuple(pltpu.VMEM(shape, jnp.float32) for shape in shapes),
        in_specs=[
            pl.BlockSpec(memory_space=pltpu.HBM),
            pl.BlockSpec(memory_space=pltpu.HBM),
            pl.BlockSpec(memory_space=pltpu.HBM),
        ],
        out_specs=(pl.BlockSpec(memory_space=pltpu.VMEM), pl.BlockSpec(memory_space=pl.ANY)),
        scratch_shapes=[
            pltpu.VMEM((F, depth, rows + 16, width), jnp.float32),
            pltpu.VMEM((2, F, depth, rows, width), jnp.float32),
            pltpu.VMEM((F, depth, rows, width), jnp.float32),
            pltpu.VMEM((F, depth, ROWS, width), jnp.float32),
            pltpu.VMEM((F, F, 8, 128), jnp.float32),
            pltpu.VMEM((F, F, 8, 128), jnp.float32),
            pltpu.VMEM((members, 2, depth, share, width), jnp.float32),
            pltpu.VMEM((F, F), jnp.float32),
            pltpu.VMEM((F, F), jnp.float32),
            pltpu.VMEM((2, F, F, 128), jnp.float32),
            dma((7,)), dma((chunks,)), dma((chunks,)), dma((chunks,)), dma((chunks,)), dma((chunks,)), dma((chunks,)),
            dma, dma, dma, regular, regular, regular,
            dma((chunks,)), regular,
        ],
        compiler_params=pltpu.CompilerParams(
            collective_id=0, has_side_effects=True, vmem_limit_bytes=40 * 1024 * 1024
        ),
    )(*arrays)
    return pl.pallas_call(
        put_out,
        out_shape=tuple(pltpu.HBM(shape, jnp.float32) for shape in shapes),
        in_specs=[pl.BlockSpec(memory_space=pltpu.VMEM)] * 2,
        out_specs=(pl.BlockSpec(memory_space=pltpu.HBM),) * 2,
        scratch_shapes=[pltpu.SemaphoreType.DMA((PARTS + 1,))],
        compiler_params=pltpu.CompilerParams(vmem_limit_bytes=1024 * 1024),
    )(*results)


def solution(mesh):
    groups, members = mesh.shape["grp"], mesh.shape["dev"]
    return jax.shard_map(
        functools.partial(per_device, groups, members),
        mesh=mesh,
        in_specs=(P(None, ("grp", "dev"), None, None), P(), P()),
        out_specs=(P(None, ("grp", "dev"), None, None), P(None, "grp", "dev", None)),
        check_vma=False,
    )
```
